8 devices in a mesh: dp: 1 (over z), x: 8 (over y, x, core).
Axes of the slice: x: 2, y: 2, z: 1, core: 2. Of those that a mesh axis runs over, the one named last changes fastest.
Arguments:
- c_raw: bfloat16 [96, 6144, 512], P('dp', 'x')
- k_raw: bfloat16 [96, 6144, 64], P('dp', 'x')
- norm_gain: bfloat16 [512], replicated
- rope_cos: float32 [6144, 32], P('x')
- rope_sin: float32 [6144, 32], P('x')
- seq_lens: int32 [96], P('dp')
- q_lat: bfloat16 [96, 128, 512], P(('dp', 'x'))
- q_rope: bfloat16 [96, 128, 64], P(('dp', 'x'))
Outputs:
- output 1: bfloat16 [96, 6144, 512], P(('dp', 'x'))
- output 2: bfloat16 [96, 6144, 64], P(('dp', 'x'))
- output 3: bfloat16 [96, 128, 512], P(('dp', 'x'))
All inputs are finite; a program needn't handle non-finite values.
Results may differ from the reference program's by a relative error of at most 0.00562413.
Values are sent between devices in bfloat16 or wider.
A program may use at most 1 GiB of HBM per device.

```python
import jax
import jax.numpy as jnp
from jax import lax

REQUESTS = 96
SEQ_LEN = 6144
KV_RANK = 512
ROPE_DIM = 64
NUM_HEADS = 128

NORM_EPS = 1e-6
ATTN_SCALE = (KV_RANK + ROPE_DIM) ** -0.5


def setup_inputs(seed: int = 0, part: int = 0) -> dict:
    part_key = jax.random.fold_in(jax.random.key(seed), part)
    keys = jax.random.split(part_key, 8)
    shared = jax.random.split(jax.random.key(seed + 1), 2)
    row_scale = jnp.exp(0.5 * jax.random.normal(keys[0], (REQUESTS, SEQ_LEN, 1), jnp.float32))
    c_raw = (jax.random.normal(keys[1], (REQUESTS, SEQ_LEN, KV_RANK), jnp.float32) * row_scale).astype(jnp.bfloat16)
    k_raw = jax.random.normal(keys[2], (REQUESTS, SEQ_LEN, ROPE_DIM), jnp.float32).astype(jnp.bfloat16)
    norm_gain = (1.0 + 0.3 * jax.random.normal(shared[0], (KV_RANK,), jnp.float32)).astype(jnp.bfloat16)
    half_dim = ROPE_DIM // 2
    log_base = jax.random.uniform(shared[1], (), jnp.float32, 9.0, 14.0)
    inv_freq = jnp.exp(-log_base * (2.0 * jnp.arange(half_dim, dtype=jnp.float32) / ROPE_DIM))
    angles = jnp.arange(SEQ_LEN, dtype=jnp.float32)[:, None] * inv_freq[None, :]
    seq_lens = jax.random.randint(keys[3], (REQUESTS,), SEQ_LEN // 8, SEQ_LEN + 1)
    full_index = jax.random.randint(keys[4], (), 0, REQUESTS)
    short_offset = jax.random.randint(keys[5], (), 1, REQUESTS)
    seq_lens = seq_lens.at[full_index].set(SEQ_LEN)
    seq_lens = seq_lens.at[(full_index + short_offset) % REQUESTS].set(SEQ_LEN // 8)
    q_lat = (1.3 * jax.random.normal(keys[6], (REQUESTS, NUM_HEADS, KV_RANK), jnp.float32)).astype(jnp.bfloat16)
    q_rope = (3.0 * jax.random.normal(keys[7], (REQUESTS, NUM_HEADS, ROPE_DIM), jnp.float32)).astype(jnp.bfloat16)
    return {"c_raw": c_raw, "k_raw": k_raw, "norm_gain": norm_gain, "rope_cos": jnp.cos(angles), "rope_sin": jnp.sin(angles), "seq_lens": seq_lens.astype(jnp.int32), "q_lat": q_lat, "q_rope": q_rope}


def reference(c_raw, k_raw, norm_gain, rope_cos, rope_sin, seq_lens, q_lat, q_rope):
    positions = jnp.arange(SEQ_LEN)
    half_dim = ROPE_DIM // 2
    gain = norm_gain.astype(jnp.float32)

    def one_request(operands):
        c_row, k_row, length, lat_row, rope_row = operands
        valid = positions < length
        lat_f32 = c_row.astype(jnp.float32)
        inv_rms = lax.rsqrt(jnp.mean(lat_f32 * lat_f32, axis=-1, keepdims=True) + NORM_EPS)
        c_norm = jnp.where(valid[:, None], lat_f32 * inv_rms * gain, 0.0).astype(jnp.bfloat16)
        key_f32 = k_row.astype(jnp.float32)
        key_lo = key_f32[:, :half_dim]
        key_hi = key_f32[:, half_dim:]
        rotated = jnp.concatenate([key_lo * rope_cos - key_hi * rope_sin, key_hi * rope_cos + key_lo * rope_sin], axis=-1)
        k_rope = jnp.where(valid[:, None], rotated, 0.0).astype(jnp.bfloat16)
        scores = jnp.dot(lat_row, c_norm.T, preferred_element_type=jnp.float32) + jnp.dot(rope_row, k_rope.T, preferred_element_type=jnp.float32)
        scores = jnp.where(valid[None, :], scores * ATTN_SCALE, -1e30)
        weights = jnp.exp(scores - jnp.max(scores, axis=-1, keepdims=True))
        out_row = jnp.dot(weights, c_norm.astype(jnp.float32)) / jnp.sum(weights, axis=-1, keepdims=True)
        return c_norm, k_rope, out_row.astype(jnp.bfloat16)

    c_cache, kr_cache, o_lat = lax.map(one_request, (c_raw, k_raw, seq_lens, q_lat, q_rope))
    return (c_cache, kr_cache, o_lat)
```

```python
import jax
import jax.numpy as jnp
from jax import lax
from jax.experimental import pallas as pl
from jax.experimental.pallas import tpu as pltpu
from jax.sharding import PartitionSpec as P

NORM_EPS = 1e-6
N = 8
REQ = 12
SEQ = 768
RANK = 512
ROPE = 64
HEADS = 128
REC = 128
NREC = SEQ // REC
ROWS = RANK // 128 * REC + ROPE
ATTN_SCALE = (RANK + ROPE) ** -0.5
GROUPS = (1, 2, 3, 3, 2, 1)
BASES = tuple(sum(GROUPS[:h]) for h in range(len(GROUPS)))


def norm_kernel(c_ref, k_ref, g_ref, cos_ref, sin_ref, *out_refs):
    gain = g_ref[...].astype(jnp.float32)
    key = k_ref[0].astype(jnp.float32)
    lo, hi = key[: ROPE // 2], key[ROPE // 2 :]
    cos, sin = cos_ref[...], sin_ref[...]
    rot = jnp.concatenate([lo * cos - hi * sin, hi * cos + lo * sin], axis=0).astype(jnp.bfloat16)

    def pack(out_ref):
        for p in range(NREC):
            out_ref[p, RANK // 128 * REC :, :] = rot[:, p * REC : (p + 1) * REC]

        def rows(p, _):
            x = c_ref[0, pl.ds(pl.multiple_of(p * REC, REC), REC), :].astype(jnp.float32)
            inv = lax.rsqrt(jnp.mean(x * x, axis=-1, keepdims=True) + NORM_EPS)
            y = (x * inv * gain).astype(jnp.bfloat16)
            for q in range(RANK // 128):
                out_ref[p, q * REC : (q + 1) * REC, :] = y[:, q * 128 : (q + 1) * 128]
            return 0

        lax.fori_loop(0, NREC, rows, 0)

    for k, out_ref in enumerate(out_refs):

        @pl.when(pl.program_id(0) == k)
        def _(out_ref=out_ref):
            pack(out_ref)


def norm_pack(h, me, c_raw, k_t, gain, cos_t, sin_t):
    count, base = GROUPS[h], BASES[h]

    def kernel(me_ref, *refs):
        norm_kernel(*refs)

    def request(k, j, me):
        return ((me[0] ^ k) * REQ + base + j, 0, 0)

    def out_spec(mine):
        return pl.BlockSpec((NREC, ROWS, 128), lambda k, j, me: (jnp.where(k < mine, 0, jnp.where(k == mine, j, count - 1)), 0, 0))

    grid_spec = pltpu.PrefetchScalarGridSpec(
        num_scalar_prefetch=1,
        grid=(N, count),
        in_specs=[
            pl.BlockSpec((1, SEQ, RANK), request),
            pl.BlockSpec((1, ROPE, SEQ), request),
            pl.BlockSpec((1, RANK), lambda k, j, me: (0, 0)),
            pl.BlockSpec((ROPE // 2, SEQ), lambda k, j, me: (0, 0)),
            pl.BlockSpec((ROPE // 2, SEQ), lambda k, j, me: (0, 0)),
        ],
        out_specs=[out_spec(k) for k in range(N)],
    )
    return pl.pallas_call(
        kernel,
        grid_spec=grid_spec,
        out_shape=[jax.ShapeDtypeStruct((count * NREC, ROWS, 128), jnp.bfloat16)] * N,
        cost_estimate=pl.CostEstimate(flops=count * N * 10**8, bytes_accessed=count * N * 1769472, transcendentals=0),
        name="norm_pack",
    )(me, c_raw, k_t, gain, cos_t, sin_t)


def attn_kernel(len_ref, me_ref, *refs):
    in_refs, (qa_ref, qr_ref) = refs[:N], refs[N : N + 2]
    c_ref, k_ref, o_ref, m_ref, l_ref, acc_ref = refs[-6:]
    step = pl.program_id(1)
    left = len_ref[pl.program_id(0)] - (me_ref[0] ^ step) * SEQ

    @pl.when(step == 0)
    def _():
        m_ref[...] = jnp.full_like(m_ref, -1e30)
        l_ref[...] = jnp.zeros_like(l_ref)
        acc_ref[...] = jnp.zeros_like(acc_ref)

    @pl.when(left <= 0)
    def _():
        c_ref[...] = jnp.zeros_like(c_ref)
        k_ref[...] = jnp.zeros_like(k_ref)

    def take(ref):
        def record(p, _):
            at = pl.ds(pl.multiple_of(p * REC, REC), REC)
            row_ok = lax.broadcasted_iota(jnp.int32, (REC, 1), 0) < left - p * REC
            for q in range(RANK // 128):
                piece = jnp.where(row_ok, ref[p, q * REC : (q + 1) * REC].astype(jnp.float32), 0.0)
                c_ref[0, at, q * 128 : (q + 1) * 128] = piece.astype(jnp.bfloat16)
            lane_ok = lax.broadcasted_iota(jnp.int32, (1, REC), 1) < left - p * REC
            key = jnp.where(lane_ok, ref[p, RANK // 128 * REC :].astype(jnp.float32), 0.0)
            k_ref[0, :, at] = key.astype(jnp.bfloat16)
            return 0

        lax.fori_loop(0, NREC, record, 0)

    for k in range(N):

        @pl.when((left > 0) & (step == k))
        def _(k=k):
            take(in_refs[k])

    @pl.when(left > 0)
    def _():
        c = c_ref[0]
        scores = lax.dot_general(qa_ref[0], c, (((1,), (1,)), ((), ())), preferred_element_type=jnp.float32)
        scores += lax.dot_general(qr_ref[0], k_ref[0], (((0,), (0,)), ((), ())), preferred_element_type=jnp.float32)
        lane_ok = lax.broadcasted_iota(jnp.int32, (1, SEQ), 1) < left
        scores = jnp.where(lane_ok, scores * ATTN_SCALE, -1e30)
        m_old = m_ref[:, :1]
        m_new = jnp.maximum(m_old, jnp.max(scores, axis=-1, keepdims=True))
        weights = jnp.exp(scores - m_new)
        decay = jnp.exp(m_old - m_new)
        l_ref[...] = jnp.broadcast_to(l_ref[:, :1] * decay + jnp.sum(weights, axis=-1, keepdims=True), l_ref.shape)
        m_ref[...] = jnp.broadcast_to(m_new, m_ref.shape)
        acc_ref[...] = acc_ref[...] * decay + jnp.dot(weights.astype(jnp.bfloat16), c, preferred_element_type=jnp.float32)

    @pl.when(step == N - 1)
    def _():
        o_ref[0] = (acc_ref[...] / l_ref[:, :1]).astype(jnp.bfloat16)


def attend(h, lens, me, parts, q_lat, q_rope_t, prev):
    count, base = GROUPS[h], BASES[h]

    def part_spec(k):
        return pl.BlockSpec((NREC, ROWS, 128), lambda j, t, lens, me: (jnp.where(t >= k, j, jnp.maximum(j - 1, 0)), 0, 0))

    in_specs = [part_spec(k) for k in range(N)] + [
        pl.BlockSpec((1, HEADS, RANK), lambda j, t, lens, me: (base + j, 0, 0)),
        pl.BlockSpec((1, ROPE, HEADS), lambda j, t, lens, me: (base + j, 0, 0)),
    ]
    operands = [lens, me, *parts, q_lat, q_rope_t]
    aliases = {}
    if prev is not None:
        in_specs += [pl.BlockSpec(memory_space=pl.ANY)] * 3
        aliases = {len(operands) + i: i for i in range(3)}
        operands += list(prev)
    grid_spec = pltpu.PrefetchScalarGridSpec(
        num_scalar_prefetch=2,
        grid=(count, N),
        in_specs=in_specs,
        out_specs=[
            pl.BlockSpec((1, SEQ, RANK), lambda j, t, lens, me: (base + j, me[0] ^ t, 0)),
            pl.BlockSpec((1, ROPE, SEQ), lambda j, t, lens, me: (base + j, 0, me[0] ^ t)),
            pl.BlockSpec((1, HEADS, RANK), lambda j, t, lens, me: (base + j, 0, 0)),
        ],
        scratch_shapes=[
            pltpu.VMEM((HEADS, 128), jnp.float32),
            pltpu.VMEM((HEADS, 128), jnp.float32),
            pltpu.VMEM((HEADS, RANK), jnp.float32),
        ],
    )
    return pl.pallas_call(
        attn_kernel,
        grid_spec=grid_spec,
        out_shape=[
            jax.ShapeDtypeStruct((REQ, N * SEQ, RANK), jnp.bfloat16),
            jax.ShapeDtypeStruct((REQ, ROPE, N * SEQ), jnp.bfloat16),
            jax.ShapeDtypeStruct((REQ, HEADS, RANK), jnp.bfloat16),
        ],
        input_output_aliases=aliases,
        cost_estimate=pl.CostEstimate(flops=count * N * 10**8, bytes_accessed=count * N * 1769472, transcendentals=0),
        name="attend",
    )(*operands)


def local_step(c_raw, k_raw, norm_gain, rope_cos, rope_sin, seq_lens, q_lat, q_rope):
    me = lax.axis_index("x")
    k_t = jnp.swapaxes(k_raw, 1, 2)
    q_rope_t = jnp.swapaxes(q_rope, 1, 2)
    own_lens = lax.dynamic_slice_in_dim(seq_lens, me * REQ, REQ)
    me_arr = me[None].astype(jnp.int32)
    arrived = []
    for h in range(len(GROUPS)):
        staged = norm_pack(h, me_arr, c_raw, k_t, norm_gain[None, :], rope_cos.T, rope_sin.T)
        arrived.append([staged[0]] + [lax.ppermute(staged[k], "x", [(s, s ^ k) for s in range(N)]) for k in range(1, N)])
    out = None
    for h, parts in enumerate(arrived):
        lens = own_lens[BASES[h] : BASES[h] + GROUPS[h]]
        out = attend(h, lens, me_arr, parts, q_lat, q_rope_t, out)
    c_cache, k_cache_t, o_lat = out
    return c_cache, jnp.swapaxes(k_cache_t, 1, 2), o_lat


def solution(mesh):
    seq_spec = P("dp", "x", None)
    req_spec = P(("dp", "x"), None, None)
    return jax.shard_map(
        local_step,
        mesh=mesh,
        in_specs=(seq_spec, seq_spec, P(None), P("x", None), P("x", None), P("dp"), req_spec, req_spec),
        out_specs=(req_spec, req_spec, req_spec),
        check_vma=False,
    )
```

```python
import jax
import jax.numpy as jnp
from jax import lax
from jax.experimental import pallas as pl
from jax.experimental.pallas import tpu as pltpu
from jax.sharding import PartitionSpec as P

NORM_EPS = 1e-6
N = 8
REQ = 12
SEQ = 768
RANK = 512
ROPE = 64
HEADS = 128
REC = 128
NREC = SEQ // REC
ROWS = RANK // 128 * REC + ROPE
ATTN_SCALE = (RANK + ROPE) ** -0.5
GROUPS = (1, 2, 3, 3, 2, 1)
BASES = tuple(sum(GROUPS[:h]) for h in range(len(GROUPS)))


def norm_kernel(c_ref, k_ref, g_ref, cos_ref, sin_ref, *out_refs):
    gain = g_ref[...].astype(jnp.float32)
    key = k_ref[0].astype(jnp.float32)
    lo, hi = key[: ROPE // 2], key[ROPE // 2 :]
    cos, sin = cos_ref[...], sin_ref[...]
    rot = jnp.concatenate([lo * cos - hi * sin, hi * cos + lo * sin], axis=0).astype(jnp.bfloat16)

    def pack(out_ref):
        for p in range(NREC):
            out_ref[p, RANK // 128 * REC :, :] = rot[:, p * REC : (p + 1) * REC]

        def rows(p, _):
            x = c_ref[0, pl.ds(pl.multiple_of(p * REC, REC), REC), :].astype(jnp.float32)
            inv = lax.rsqrt(jnp.mean(x * x, axis=-1, keepdims=True) + NORM_EPS)
            y = (x * inv * gain).astype(jnp.bfloat16)
            for q in range(RANK // 128):
                out_ref[p, q * REC : (q + 1) * REC, :] = y[:, q * 128 : (q + 1) * 128]
            return 0

        lax.fori_loop(0, NREC, rows, 0)

    for k, out_ref in enumerate(out_refs):

        @pl.when(pl.program_id(0) == k)
        def _(out_ref=out_ref):
            pack(out_ref)


def norm_pack(h, me, c_raw, k_t, gain, cos_t, sin_t, after):
    count, base = GROUPS[h], BASES[h]

    def kernel(me_ref, *refs):
        norm_kernel(*refs[:5], *refs[6:])

    def request(k, j, me):
        return ((me[0] ^ k) * REQ + base + j, 0, 0)

    def out_spec(mine):
        return pl.BlockSpec((NREC, ROWS, 128), lambda k, j, me: (jnp.where(k < mine, 0, jnp.where(k == mine, j, count - 1)), 0, 0))

    grid_spec = pltpu.PrefetchScalarGridSpec(
        num_scalar_prefetch=1,
        grid=(N, count),
        in_specs=[
            pl.BlockSpec((1, SEQ, RANK), request),
            pl.BlockSpec((1, ROPE, SEQ), request),
            pl.BlockSpec((1, RANK), lambda k, j, me: (0, 0)),
            pl.BlockSpec((ROPE // 2, SEQ), lambda k, j, me: (0, 0)),
            pl.BlockSpec((ROPE // 2, SEQ), lambda k, j, me: (0, 0)),
            pl.BlockSpec(memory_space=pl.ANY),
        ],
        out_specs=[out_spec(k) for k in range(N)],
    )
    return pl.pallas_call(
        kernel,
        grid_spec=grid_spec,
        out_shape=[jax.ShapeDtypeStruct((count * NREC, ROWS, 128), jnp.bfloat16)] * N,
        cost_estimate=pl.CostEstimate(flops=count * N * 10**8, bytes_accessed=count * N * 1769472, transcendentals=0),
        name="norm_pack",
    )(me, c_raw, k_t, gain, cos_t, sin_t, after)


def attn_kernel(len_ref, me_ref, *refs):
    in_refs, (qa_ref, qr_ref) = refs[:N], refs[N : N + 2]
    c_ref, k_ref, o_ref, m_ref, l_ref, acc_ref = refs[-6:]
    step = pl.program_id(1)
    left = len_ref[pl.program_id(0)] - (me_ref[0] ^ step) * SEQ

    @pl.when(step == 0)
    def _():
        m_ref[...] = jnp.full_like(m_ref, -1e30)
        l_ref[...] = jnp.zeros_like(l_ref)
        acc_ref[...] = jnp.zeros_like(acc_ref)

    @pl.when(left <= 0)
    def _():
        c_ref[...] = jnp.zeros_like(c_ref)
        k_ref[...] = jnp.zeros_like(k_ref)

    def take(ref):
        def record(p, _):
            at = pl.ds(pl.multiple_of(p * REC, REC), REC)
            row_ok = lax.broadcasted_iota(jnp.int32, (REC, 1), 0) < left - p * REC
            for q in range(RANK // 128):
                piece = jnp.where(row_ok, ref[p, q * REC : (q + 1) * REC].astype(jnp.float32), 0.0)
                c_ref[0, at, q * 128 : (q + 1) * 128] = piece.astype(jnp.bfloat16)
            lane_ok = lax.broadcasted_iota(jnp.int32, (1, REC), 1) < left - p * REC
            key = jnp.where(lane_ok, ref[p, RANK // 128 * REC :].astype(jnp.float32), 0.0)
            k_ref[0, :, at] = key.astype(jnp.bfloat16)
            return 0

        lax.fori_loop(0, NREC, record, 0)

    for k in range(N):

        @pl.when((left > 0) & (step == k))
        def _(k=k):
            take(in_refs[k])

    @pl.when(left > 0)
    def _():
        c = c_ref[0]
        scores = lax.dot_general(qa_ref[0], c, (((1,), (1,)), ((), ())), preferred_element_type=jnp.float32)
        scores += lax.dot_general(qr_ref[0], k_ref[0], (((0,), (0,)), ((), ())), preferred_element_type=jnp.float32)
        lane_ok = lax.broadcasted_iota(jnp.int32, (1, SEQ), 1) < left
        scores = jnp.where(lane_ok, scores * ATTN_SCALE, -1e30)
        m_old = m_ref[:, :1]
        m_new = jnp.maximum(m_old, jnp.max(scores, axis=-1, keepdims=True))
        weights = jnp.exp(scores - m_new)
        decay = jnp.exp(m_old - m_new)
        l_ref[...] = jnp.broadcast_to(l_ref[:, :1] * decay + jnp.sum(weights, axis=-1, keepdims=True), l_ref.shape)
        m_ref[...] = jnp.broadcast_to(m_new, m_ref.shape)
        acc_ref[...] = acc_ref[...] * decay + jnp.dot(weights.astype(jnp.bfloat16), c, preferred_element_type=jnp.float32)

    @pl.when(step == N - 1)
    def _():
        o_ref[0] = (acc_ref[...] / l_ref[:, :1]).astype(jnp.bfloat16)


def attend(h, lens, me, parts, q_lat, q_rope_t, prev):
    count, base = GROUPS[h], BASES[h]

    def part_spec(k):
        return pl.BlockSpec((NREC, ROWS, 128), lambda j, t, lens, me: (jnp.where(t >= k, j, jnp.maximum(j - 1, 0)), 0, 0))

    in_specs = [part_spec(k) for k in range(N)] + [
        pl.BlockSpec((1, HEADS, RANK), lambda j, t, lens, me: (base + j, 0, 0)),
        pl.BlockSpec((1, ROPE, HEADS), lambda j, t, lens, me: (base + j, 0, 0)),
    ]
    operands = [lens, me, *parts, q_lat, q_rope_t]
    aliases = {}
    if prev is not None:
        in_specs += [pl.BlockSpec(memory_space=pl.ANY)] * 3
        aliases = {len(operands) + i: i for i in range(3)}
        operands += list(prev)
    grid_spec = pltpu.PrefetchScalarGridSpec(
        num_scalar_prefetch=2,
        grid=(count, N),
        in_specs=in_specs,
        out_specs=[
            pl.BlockSpec((1, SEQ, RANK), lambda j, t, lens, me: (base + j, me[0] ^ t, 0)),
            pl.BlockSpec((1, ROPE, SEQ), lambda j, t, lens, me: (base + j, 0, me[0] ^ t)),
            pl.BlockSpec((1, HEADS, RANK), lambda j, t, lens, me: (base + j, 0, 0)),
        ],
        scratch_shapes=[
            pltpu.VMEM((HEADS, 128), jnp.float32),
            pltpu.VMEM((HEADS, 128), jnp.float32),
            pltpu.VMEM((HEADS, RANK), jnp.float32),
        ],
    )
    return pl.pallas_call(
        attn_kernel,
        grid_spec=grid_spec,
        out_shape=[
            jax.ShapeDtypeStruct((REQ, N * SEQ, RANK), jnp.bfloat16),
            jax.ShapeDtypeStruct((REQ, ROPE, N * SEQ), jnp.bfloat16),
            jax.ShapeDtypeStruct((REQ, HEADS, RANK), jnp.bfloat16),
        ],
        input_output_aliases=aliases,
        cost_estimate=pl.CostEstimate(flops=count * N * 10**8, bytes_accessed=count * N * 1769472, transcendentals=0),
        name="attend",
    )(*operands)


def local_step(c_raw, k_raw, norm_gain, rope_cos, rope_sin, seq_lens, q_lat, q_rope):
    me = lax.axis_index("x")
    k_t = jnp.swapaxes(k_raw, 1, 2)
    q_rope_t = jnp.swapaxes(q_rope, 1, 2)
    own_lens = lax.dynamic_slice_in_dim(seq_lens, me * REQ, REQ)
    me_arr = me[None].astype(jnp.int32)
    arrived = []
    after = norm_gain[None, :]
    for h in range(len(GROUPS)):
        staged = norm_pack(h, me_arr, c_raw, k_t, norm_gain[None, :], rope_cos.T, rope_sin.T, after)
        after = staged[0]
        arrived.append([staged[0]] + [lax.ppermute(staged[k], "x", [(s, s ^ k) for s in range(N)]) for k in range(1, N)])
    out = None
    for h, parts in enumerate(arrived):
        lens = own_lens[BASES[h] : BASES[h] + GROUPS[h]]
        out = attend(h, lens, me_arr, parts, q_lat, q_rope_t, out)
    c_cache, k_cache_t, o_lat = out
    return c_cache, jnp.swapaxes(k_cache_t, 1, 2), o_lat


def solution(mesh):
    seq_spec = P("dp", "x", None)
    req_spec = P(("dp", "x"), None, None)
    return jax.shard_map(
        local_step,
        mesh=mesh,
        in_specs=(seq_spec, seq_spec, P(None), P("x", None), P("x", None), P("dp"), req_spec, req_spec),
        out_specs=(req_spec, req_spec, req_spec),
        check_vma=False,
    )
```

```python
import jax
import jax.numpy as jnp
from jax import lax
from jax.experimental import pallas as pl
from jax.experimental.pallas import tpu as pltpu
from jax.sharding import PartitionSpec as P

NORM_EPS = 1e-6
N = 8
REQ = 12
SEQ = 768
RANK = 512
ROPE = 64
HEADS = 128
REC = 128
NREC = SEQ // REC
ROWS = RANK // 128 * REC + ROPE
ATTN_SCALE = (RANK + ROPE) ** -0.5
GROUPS = (1, 1, 2, 2, 2, 2, 1, 1)
DEPTH = 2
BASES = tuple(sum(GROUPS[:h]) for h in range(len(GROUPS)))


def norm_kernel(c_ref, k_ref, g_ref, cos_ref, sin_ref, *out_refs):
    gain = g_ref[...].astype(jnp.float32)
    key = k_ref[0].astype(jnp.float32)
    lo, hi = key[: ROPE // 2], key[ROPE // 2 :]
    cos, sin = cos_ref[...], sin_ref[...]
    rot = jnp.concatenate([lo * cos - hi * sin, hi * cos + lo * sin], axis=0).astype(jnp.bfloat16)

    def pack(out_ref):
        for p in range(NREC):
            out_ref[p, RANK // 128 * REC :, :] = rot[:, p * REC : (p + 1) * REC]

        def rows(p, _):
            x = c_ref[0, pl.ds(pl.multiple_of(p * REC, REC), REC), :].astype(jnp.float32)
            inv = lax.rsqrt(jnp.mean(x * x, axis=-1, keepdims=True) + NORM_EPS)
            y = (x * inv * gain).astype(jnp.bfloat16)
            for q in range(RANK // 128):
                out_ref[p, q * REC : (q + 1) * REC, :] = y[:, q * 128 : (q + 1) * 128]
            return 0

        lax.fori_loop(0, NREC, rows, 0)

    for k, out_ref in enumerate(out_refs):

        @pl.when(pl.program_id(0) == k)
        def _(out_ref=out_ref):
            pack(out_ref)


def norm_pack(h, me, c_raw, k_t, gain, cos_t, sin_t, after):
    count, base = GROUPS[h], BASES[h]

    def kernel(me_ref, *refs):
        norm_kernel(*refs[:5], *refs[6:])

    def request(k, j, me):
        return ((me[0] ^ k) * REQ + base + j, 0, 0)

    def out_spec(mine):
        return pl.BlockSpec((NREC, ROWS, 128), lambda k, j, me: (jnp.where(k < mine, 0, jnp.where(k == mine, j, count - 1)), 0, 0))

    grid_spec = pltpu.PrefetchScalarGridSpec(
        num_scalar_prefetch=1,
        grid=(N, count),
        in_specs=[
            pl.BlockSpec((1, SEQ, RANK), request),
            pl.BlockSpec((1, ROPE, SEQ), request),
            pl.BlockSpec((1, RANK), lambda k, j, me: (0, 0)),
            pl.BlockSpec((ROPE // 2, SEQ), lambda k, j, me: (0, 0)),
            pl.BlockSpec((ROPE // 2, SEQ), lambda k, j, me: (0, 0)),
            pl.BlockSpec(memory_space=pl.ANY),
        ],
        out_specs=[out_spec(k) for k in range(N)],
    )
    return pl.pallas_call(
        kernel,
        grid_spec=grid_spec,
        out_shape=[jax.ShapeDtypeStruct((count * NREC, ROWS, 128), jnp.bfloat16)] * N,
        cost_estimate=pl.CostEstimate(flops=count * N * 10**8, bytes_accessed=count * N * 1769472, transcendentals=0),
        name="norm_pack",
    )(me, c_raw, k_t, gain, cos_t, sin_t, after)


def attn_kernel(len_ref, me_ref, *refs):
    in_refs, (qa_ref, qr_ref) = refs[:N], refs[N : N + 2]
    c_ref, k_ref, o_ref, m_ref, l_ref, acc_ref = refs[-6:]
    step = pl.program_id(1)
    left = len_ref[pl.program_id(0)] - (me_ref[0] ^ step) * SEQ

    @pl.when(step == 0)
    def _():
        m_ref[...] = jnp.full_like(m_ref, -1e30)
        l_ref[...] = jnp.zeros_like(l_ref)
        acc_ref[...] = jnp.zeros_like(acc_ref)

    @pl.when(left <= 0)
    def _():
        c_ref[...] = jnp.zeros_like(c_ref)
        k_ref[...] = jnp.zeros_like(k_ref)

    def take(ref):
        def record(p, _):
            at = pl.ds(pl.multiple_of(p * REC, REC), REC)
            row_ok = lax.broadcasted_iota(jnp.int32, (REC, 1), 0) < left - p * REC
            for q in range(RANK // 128):
                piece = jnp.where(row_ok, ref[p, q * REC : (q + 1) * REC].astype(jnp.float32), 0.0)
                c_ref[0, at, q * 128 : (q + 1) * 128] = piece.astype(jnp.bfloat16)
            lane_ok = lax.broadcasted_iota(jnp.int32, (1, REC), 1) < left - p * REC
            key = jnp.where(lane_ok, ref[p, RANK // 128 * REC :].astype(jnp.float32), 0.0)
            k_ref[0, :, at] = key.astype(jnp.bfloat16)
            return 0

        lax.fori_loop(0, NREC, record, 0)

    for k in range(N):

        @pl.when((left > 0) & (step == k))
        def _(k=k):
            take(in_refs[k])

    @pl.when(left > 0)
    def _():
        c = c_ref[0]
        scores = lax.dot_general(qa_ref[0], c, (((1,), (1,)), ((), ())), preferred_element_type=jnp.float32)
        scores += lax.dot_general(qr_ref[0], k_ref[0], (((0,), (0,)), ((), ())), preferred_element_type=jnp.float32)
        lane_ok = lax.broadcasted_iota(jnp.int32, (1, SEQ), 1) < left
        scores = jnp.where(lane_ok, scores * ATTN_SCALE, -1e30)
        m_old = m_ref[:, :1]
        m_new = jnp.maximum(m_old, jnp.max(scores, axis=-1, keepdims=True))
        weights = jnp.exp(scores - m_new)
        decay = jnp.exp(m_old - m_new)
        l_ref[...] = jnp.broadcast_to(l_ref[:, :1] * decay + jnp.sum(weights, axis=-1, keepdims=True), l_ref.shape)
        m_ref[...] = jnp.broadcast_to(m_new, m_ref.shape)
        acc_ref[...] = acc_ref[...] * decay + jnp.dot(weights.astype(jnp.bfloat16), c, preferred_element_type=jnp.float32)

    @pl.when(step == N - 1)
    def _():
        o_ref[0] = (acc_ref[...] / l_ref[:, :1]).astype(jnp.bfloat16)


def attend(h, lens, me, parts, q_lat, q_rope_t, prev):
    count, base = GROUPS[h], BASES[h]

    def part_spec(k):
        return pl.BlockSpec((NREC, ROWS, 128), lambda j, t, lens, me: (jnp.where(t >= k, j, jnp.maximum(j - 1, 0)), 0, 0))

    in_specs = [part_spec(k) for k in range(N)] + [
        pl.BlockSpec((1, HEADS, RANK), lambda j, t, lens, me: (base + j, 0, 0)),
        pl.BlockSpec((1, ROPE, HEADS), lambda j, t, lens, me: (base + j, 0, 0)),
    ]
    operands = [lens, me, *parts, q_lat, q_rope_t]
    aliases = {}
    if prev is not None:
        in_specs += [pl.BlockSpec(memory_space=pl.ANY)] * 3
        aliases = {len(operands) + i: i for i in range(3)}
        operands += list(prev)
    grid_spec = pltpu.PrefetchScalarGridSpec(
        num_scalar_prefetch=2,
        grid=(count, N),
        in_specs=in_specs,
        out_specs=[
            pl.BlockSpec((1, SEQ, RANK), lambda j, t, lens, me: (base + j, me[0] ^ t, 0)),
            pl.BlockSpec((1, ROPE, SEQ), lambda j, t, lens, me: (base + j, 0, me[0] ^ t)),
            pl.BlockSpec((1, HEADS, RANK), lambda j, t, lens, me: (base + j, 0, 0)),
        ],
        scratch_shapes=[
            pltpu.VMEM((HEADS, 128), jnp.float32),
            pltpu.VMEM((HEADS, 128), jnp.float32),
            pltpu.VMEM((HEADS, RANK), jnp.float32),
        ],
    )
    return pl.pallas_call(
        attn_kernel,
        grid_spec=grid_spec,
        out_shape=[
            jax.ShapeDtypeStruct((REQ, N * SEQ, RANK), jnp.bfloat16),
            jax.ShapeDtypeStruct((REQ, ROPE, N * SEQ), jnp.bfloat16),
            jax.ShapeDtypeStruct((REQ, HEADS, RANK), jnp.bfloat16),
        ],
        input_output_aliases=aliases,
        cost_estimate=pl.CostEstimate(flops=count * N * 10**8, bytes_accessed=count * N * 1769472, transcendentals=0),
        name="attend",
    )(*operands)


def local_step(c_raw, k_raw, norm_gain, rope_cos, rope_sin, seq_lens, q_lat, q_rope):
    me = lax.axis_index("x")
    k_t = jnp.swapaxes(k_raw, 1, 2)
    q_rope_t = jnp.swapaxes(q_rope, 1, 2)
    own_lens = lax.dynamic_slice_in_dim(seq_lens, me * REQ, REQ)
    me_arr = me[None].astype(jnp.int32)
    arrived = []
    after = norm_gain[None, :]
    for h in range(len(GROUPS)):
        staged = norm_pack(h, me_arr, c_raw, k_t, norm_gain[None, :], rope_cos.T, rope_sin.T, after)
        after = staged[0]
        if h >= DEPTH:
            sends, arrived[h - DEPTH][1:] = lax.optimization_barrier((staged[1:], arrived[h - DEPTH][1:]))
            staged = [staged[0], *sends]
        arrived.append([staged[0]] + [lax.ppermute(staged[k], "x", [(s, s ^ k) for s in range(N)]) for k in range(1, N)])
    out = None
    for h, parts in enumerate(arrived):
        lens = own_lens[BASES[h] : BASES[h] + GROUPS[h]]
        out = attend(h, lens, me_arr, parts, q_lat, q_rope_t, out)
    c_cache, k_cache_t, o_lat = out
    return c_cache, jnp.swapaxes(k_cache_t, 1, 2), o_lat


def solution(mesh):
    seq_spec = P("dp", "x", None)
    req_spec = P(("dp", "x"), None, None)
    return jax.shard_map(
        local_step,
        mesh=mesh,
        in_specs=(seq_spec, seq_spec, P(None), P("x", None), P("x", None), P("dp"), req_spec, req_spec),
        out_specs=(req_spec, req_spec, req_spec),
        check_vma=False,
    )
```

```python
import jax
import jax.numpy as jnp
import numpy as np
from jax import lax
from jax.experimental import pallas as pl
from jax.experimental.pallas import tpu as pltpu
from jax.sharding import PartitionSpec as P

NORM_EPS = 1e-6
N = 8
CHIPS = 4
REQ = 12
SEQ = 768
RANK = 512
ROPE = 64
HEADS = 128
UNIT = 256
PER = SEQ // UNIT
PIECES = RANK // 128
HALVES = UNIT // 128
ROWS = PIECES * UNIT + HALVES * ROPE
SLOTS = 2 * REQ * PER
NONE = 10**6
ATTN_SCALE = (RANK + ROPE) ** -0.5
DEPTH = 2
LAG = 4


class Plan:
    def __init__(self, chunks):
        self.chunks = chunks
        self.starts = np.cumsum([0] + [c[0] for c in chunks])[:-1]
        assert sum(c[0] for c in chunks) == SLOTS
        self.slot = np.full((N, CHIPS, SLOTS), NONE, np.int32)
        self.cap = np.zeros((N, CHIPS), np.int32)
        for s in range(N):
            for q in range(CHIPS):
                for (width, _, cross, along), start in zip(chunks, self.starts):
                    if q == 0 or s in (along if q == 1 else cross):
                        self.slot[s, q, start : start + width] = self.cap[s, q] + np.arange(width)
                        self.cap[s, q] += width


ALL = (0, 1, 2, 3, 4, 5, 6, 7)
UP = (0, 1, 2, 3)


def tight_plan():
    early, mid, late = ALL, (0, 1, 2, 3, 4, 5, 6), (0, 1, 2, 3, 4, 5)
    both, one = (0, 1, 4, 5, 6, 7), (0, 1, 2, 4, 5, 6, 7)
    return Plan([
        (4, "direct", early, early),
        (8, "direct", early, early),
        (7, "relay", UP, UP),
        (5, "direct", both, early),
        (7, "relay", UP, UP),
        (5, "direct", both, early),
        (6, "direct", one, early),
        (8, "direct", mid, mid),
        (8, "direct", late, late),
        (8, "direct", late, late),
        (4, "direct", (0, 1, 2, 3, 4), (0, 1, 2, 3, 4)),
        (2, "direct", (0, 1, 2, 3, 4), (0, 1, 2, 3, 4)),
    ])


def loose_plan():
    early, mid, late = ALL, (0, 1, 2, 3, 4, 5, 6), (0, 1, 2, 3, 4, 5)
    both, one = (0, 1, 4, 5, 6, 7), (0, 1, 2, 4, 5, 6, 7)
    return Plan([
        (4, "direct", early, early),
        (8, "direct", early, early),
        (6, "relay", UP, UP),
        (6, "direct", both, early),
        (4, "relay", UP, UP),
        (6, "direct", one, early),
        (8, "direct", early, early),
        (8, "direct", mid, mid),
        (8, "direct", late, late),
        (8, "direct", late, late),
        (4, "direct", UP, UP),
        (2, "direct", UP, UP),
    ])


def full_plan():
    return Plan([(width, "direct", ALL, ALL) for width in (4, 8, 8, 8, 8, 8, 8, 8, 8, 4)])


PLANS = (tight_plan(), loose_plan(), full_plan())


def norm_pack(width, start, tabs, c_raw, k_t, gain, cos_t, sin_t, after):
    def kernel(req_ref, unit_ref, ok_ref, c_ref, k_ref, g_ref, cos_ref, sin_ref, *refs):
        outs = refs[-CHIPS:]

        def pack(out_ref):
            key = k_ref[0].astype(jnp.float32)
            lo, hi = key[: ROPE // 2], key[ROPE // 2 :]
            cos, sin = cos_ref[...], sin_ref[...]
            rot = jnp.concatenate([lo * cos - hi * sin, hi * cos + lo * sin], axis=0).astype(jnp.bfloat16)
            for p in range(HALVES):
                at = PIECES * UNIT + p * ROPE
                out_ref[0, at : at + ROPE, :] = rot[:, p * 128 : (p + 1) * 128]
                x = c_ref[0, p * 128 : (p + 1) * 128, :].astype(jnp.float32)
                inv = lax.rsqrt(jnp.mean(x * x, axis=-1, keepdims=True) + NORM_EPS)
                y = (x * inv * g_ref[...].astype(jnp.float32)).astype(jnp.bfloat16)
                for i in range(PIECES):
                    at = i * UNIT + p * 128
                    out_ref[0, at : at + 128, :] = y[:, i * 128 : (i + 1) * 128]

        q = pl.program_id(0)
        ok = ok_ref[q * SLOTS + start + pl.program_id(1)] > 0
        for mine in range(CHIPS):

            @pl.when(ok & (q == mine))
            def _(mine=mine):
                pack(outs[mine])

    def out_spec(mine):
        return pl.BlockSpec((1, ROWS, 128), lambda q, j, *_: (jnp.where(q < mine, 0, jnp.where(q == mine, j, width - 1)), 0, 0))

    def at(q, j):
        return q * SLOTS + start + j

    grid_spec = pltpu.PrefetchScalarGridSpec(
        num_scalar_prefetch=3,
        grid=(CHIPS, width),
        in_specs=[
            pl.BlockSpec((1, UNIT, RANK), lambda q, j, req, unit, ok: (req[at(q, j)], unit[at(q, j)], 0)),
            pl.BlockSpec((1, ROPE, UNIT), lambda q, j, req, unit, ok: (req[at(q, j)], 0, unit[at(q, j)])),
            pl.BlockSpec((1, RANK), lambda q, j, *_: (0, 0)),
            pl.BlockSpec((ROPE // 2, UNIT), lambda q, j, req, unit, ok: (0, unit[at(q, j)])),
            pl.BlockSpec((ROPE // 2, UNIT), lambda q, j, req, unit, ok: (0, unit[at(q, j)])),
        ]
        + [pl.BlockSpec(memory_space=pl.ANY)] * len(after),
        out_specs=[out_spec(q) for q in range(CHIPS)],
    )
    return pl.pallas_call(
        kernel,
        grid_spec=grid_spec,
        out_shape=[jax.ShapeDtypeStruct((width, ROWS, 128), jnp.bfloat16)] * CHIPS,
        cost_estimate=pl.CostEstimate(flops=width * 10**8, bytes_accessed=width * 4 * 589824, transcendentals=0),
        name="norm_pack",
    )(*tabs, c_raw, k_t, gain, cos_t, sin_t, *after)


def attend(width, start, first, last, tabs, parts, q_lat, q_rope_t, caches, state):
    def kernel(left_ref, req_ref, pos_ref, *refs):
        in_refs, (qa_ref, qr_ref) = refs[:N], refs[N : N + 2]
        old_ref = None if first else refs[N + 4]
        outs = refs[N + (4 if first else 5) :]
        c_ref, k_ref, st_ref = outs[:3]
        a, j = pl.program_id(0), pl.program_id(1)
        n = N * start + a * width + j
        left = left_ref[n]

        @pl.when((a == 0) & (j == 0))
        def _():
            if first:
                st_ref[:, :, : RANK + 128] = jnp.zeros((REQ, HEADS, RANK + 128), jnp.float32)
                st_ref[:, :, RANK + 128 :] = jnp.full((REQ, HEADS, 128), -1e30, jnp.float32)
            else:
                st_ref[...] = old_ref[...]

        row_ok = lax.broadcasted_iota(jnp.int32, (UNIT, 1), 0) < left
        lane_ok = lax.broadcasted_iota(jnp.int32, (1, UNIT), 1) < left

        for k in range(N):

            @pl.when((left > 0) & (a == k))
            def _(ref=in_refs[k]):
                for i in range(PIECES):
                    piece = jnp.where(row_ok, ref[0, i * UNIT : (i + 1) * UNIT, :].astype(jnp.float32), 0.0)
                    c_ref[0, :, i * 128 : (i + 1) * 128] = piece.astype(jnp.bfloat16)
                for p in range(HALVES):
                    base = PIECES * UNIT + p * ROPE
                    key = jnp.where(lane_ok[:, p * 128 : (p + 1) * 128], ref[0, base : base + ROPE, :].astype(jnp.float32), 0.0)
                    k_ref[0, :, p * 128 : (p + 1) * 128] = key.astype(jnp.bfloat16)

        @pl.when(left > 0)
        def _():
            r = req_ref[n]
            c = c_ref[0]
            scores = lax.dot_general(qa_ref[r], c, (((1,), (1,)), ((), ())), preferred_element_type=jnp.float32)
            scores += lax.dot_general(qr_ref[r], k_ref[0], (((0,), (0,)), ((), ())), preferred_element_type=jnp.float32)
            scores = jnp.where(lane_ok, scores * ATTN_SCALE, -1e30)
            l_old = st_ref[r, :, RANK : RANK + 1]
            m_old = st_ref[r, :, RANK + 128 : RANK + 129]
            m_new = jnp.maximum(m_old, jnp.max(scores, axis=-1, keepdims=True))
            weights = jnp.exp(scores - m_new)
            decay = jnp.exp(m_old - m_new)
            l_new = l_old * decay + jnp.sum(weights, axis=-1, keepdims=True)
            st_ref[r, :, RANK : RANK + 128] = jnp.broadcast_to(l_new, (HEADS, 128))
            st_ref[r, :, RANK + 128 :] = jnp.broadcast_to(m_new, (HEADS, 128))
            st_ref[r, :, :RANK] = st_ref[r, :, :RANK] * decay + jnp.dot(
                weights.astype(jnp.bfloat16), c, preferred_element_type=jnp.float32
            )

        if last:
            o_ref = outs[3]

            @pl.when((a == N - 1) & (j == width - 1))
            def _():
                def finish(r, _):
                    o_ref[r] = (st_ref[r, :, :RANK] / st_ref[r, :, RANK : RANK + 1]).astype(jnp.bfloat16)
                    return 0

                lax.fori_loop(0, REQ, finish, 0)

    def part_spec(mine):
        return pl.BlockSpec((1, ROWS, 128), lambda a, j, *_: (jnp.where(a < mine, 0, jnp.where(a == mine, j, width - 1)), 0, 0))

    def at(a, j):
        return N * start + a * width + j

    whole = lambda shape: pl.BlockSpec(shape, lambda a, j, *_: (0,) * len(shape))
    state_shape = (REQ, HEADS, RANK + 256)
    in_specs = [part_spec(k) for k in range(N)] + [whole((REQ, HEADS, RANK)), whole((REQ, ROPE, HEADS))]
    in_specs += [pl.BlockSpec(memory_space=pl.ANY)] * 2
    operands = [*tabs, *parts, q_lat, q_rope_t]
    aliases = {len(operands): 0, len(operands) + 1: 1}
    operands += list(caches)
    if not first:
        in_specs.append(whole(state_shape))
        aliases[len(operands)] = 2
        operands.append(state)
    out_specs = [
        pl.BlockSpec((1, UNIT, RANK), lambda a, j, left, req, pos: (req[at(a, j)], pos[at(a, j)], 0)),
        pl.BlockSpec((1, ROPE, UNIT), lambda a, j, left, req, pos: (req[at(a, j)], 0, pos[at(a, j)])),
        whole(state_shape),
    ]
    out_shape = [jax.ShapeDtypeStruct(c.shape, c.dtype) for c in caches] + [jax.ShapeDtypeStruct(state_shape, jnp.float32)]
    if last:
        out_specs.append(whole((REQ, HEADS, RANK)))
        out_shape.append(jax.ShapeDtypeStruct((REQ, HEADS, RANK), jnp.bfloat16))
    return pl.pallas_call(
        kernel,
        grid_spec=pltpu.PrefetchScalarGridSpec(num_scalar_prefetch=3, grid=(N, width), in_specs=in_specs, out_specs=out_specs),
        out_shape=out_shape,
        input_output_aliases=aliases,
        cost_estimate=pl.CostEstimate(flops=width * 2 * 10**8, bytes_accessed=width * 8 * 589824, transcendentals=0),
        name="attend",
    )(*operands)


def blank_caches():
    def kernel(c_ref, k_ref):
        c_ref[...] = jnp.zeros_like(c_ref)
        k_ref[...] = jnp.zeros_like(k_ref)

    return pl.pallas_call(
        kernel,
        grid=(REQ, N),
        out_specs=[pl.BlockSpec((1, SEQ, RANK), lambda r, s: (r, s, 0)), pl.BlockSpec((1, ROPE, SEQ), lambda r, s: (r, 0, s))],
        out_shape=[
            jax.ShapeDtypeStruct((REQ, N * SEQ, RANK), jnp.bfloat16),
            jax.ShapeDtypeStruct((REQ, ROPE, N * SEQ), jnp.bfloat16),
        ],
        cost_estimate=pl.CostEstimate(flops=4 * 10**8, bytes_accessed=85 * 10**6, transcendentals=0),
        name="blank",
    )()


def count_units(seq_lens):
    valid = jnp.clip(seq_lens[None, :] - SEQ * jnp.arange(N, dtype=jnp.int32)[:, None], 0, SEQ)
    left = valid.reshape(N, CHIPS, 2, REQ)[..., None] - UNIT * jnp.arange(PER, dtype=jnp.int32)
    left = left.transpose(0, 1, 3, 4, 2).reshape(N, CHIPS, SLOTS)
    return left


def split_place(place):
    return place // (2 * PER), place // 2 % PER, place % 2


def run_plan(plan, me, left, c_raw, k_t, gain, cos_t, sin_t, q_lat, q_rope_t):
    chip = me // 2
    have = left > 0
    rank = jnp.cumsum(have.astype(jnp.int32), axis=-1)
    places = jnp.arange(SLOTS, dtype=jnp.int32)

    chips = chip ^ jnp.arange(CHIPS)
    mine = rank[me][chips]
    slot = jnp.asarray(plan.slot)[me]
    place = jnp.sum((mine[:, None, :] <= slot[:, :, None]).astype(jnp.int32), axis=-1)
    final = jnp.max(jnp.where(have[me][chips], places, 0), axis=-1, keepdims=True)
    held = jnp.minimum(place, final)
    req, unit, core = split_place(held)
    pack_tabs = [
        ((2 * chips[:, None] + core) * REQ + req).reshape(-1),
        unit.reshape(-1),
        (place < SLOTS).astype(jnp.int32).reshape(-1),
    ]

    part = jnp.arange(N)
    source = me ^ part
    theirs = rank[source, chip]
    slot = jnp.asarray(plan.slot)[source, part // 2]
    place = jnp.sum((theirs[:, None, :] <= slot[:, :, None]).astype(jnp.int32), axis=-1)
    req, unit, core = split_place(place)
    rows = jnp.sum(jnp.where(place[:, :, None] == places, left[source, chip][:, None, :], 0), axis=-1)
    rows = jnp.where(core == me % 2, jnp.minimum(rows, UNIT), 0)
    code = req * 64 + source[:, None] * PER + unit
    order = lambda t: jnp.concatenate([t[:, s : s + c[0]].reshape(-1) for c, s in zip(plan.chunks, plan.starts)])
    rows, code = order(rows), order(code)
    steps = jnp.arange(N * SLOTS, dtype=jnp.int32)
    chunk_of = np.repeat(np.arange(len(plan.chunks)), [N * c[0] for c in plan.chunks]).astype(np.int32)
    same = jnp.asarray(chunk_of)[:, None] == jnp.asarray(chunk_of)[None, :]
    key = jnp.where(rows > 0, steps * 1024 + code, -1)
    before = jnp.max(jnp.where(same & (steps[None, :] <= steps[:, None]), key[None, :], -1), axis=-1)
    ahead = jnp.min(jnp.where(same & (key >= 0)[None, :], key[None, :], N * SLOTS * 1024), axis=-1)
    code = jnp.where(before >= 0, before, ahead) % 1024
    attend_tabs = [rows, code // 64, code % 64]

    pairs = lambda sources, hop: [(s, s ^ hop) for s in sources]
    send = lambda x, pairs: lax.ppermute(x, "x", pairs)
    caches = blank_caches()
    state = out = None
    landed, parts, done = [], [], []
    count = len(plan.chunks)

    def finish(c):
        nonlocal caches, state, out
        width = plan.chunks[c][0]
        got = attend(width, int(plan.starts[c]), c == 0, c == count - 1, attend_tabs, parts[c], q_lat, q_rope_t, caches, state)
        caches, state = got[:2], got[2]
        if c == count - 1:
            out = got[3]

    after = []
    for c, (width, kind, cross, along) in enumerate(plan.chunks):
        if c >= LAG:
            finish(c - LAG)
            after = after + [state]
        staged = norm_pack(width, int(plan.starts[c]), pack_tabs, c_raw, k_t, gain, cos_t, sin_t, after)
        after = [staged[0]]
        sends = list(staged)
        if c >= DEPTH:
            sends, landed[c - DEPTH] = lax.optimization_barrier((sends, landed[c - DEPTH]))
        own = sends[0]
        far = send(sends[3], pairs(UP, 4) if kind == "relay" else pairs(cross, 6))
        near = send(sends[1], pairs(along, 2))
        over = send(sends[2], pairs(cross, 4))
        landed.append([near, over, far])
        twin = send(own, pairs(ALL, 1))
        parts.append([own, twin])
        heads = lambda sources, hop: [s ^ hop for s in sources]
        if kind == "relay":
            far = send(far, pairs((4, 5, 6, 7), 2))
            far_heads = (4, 5, 6, 7)
        else:
            far_heads = heads(cross, 6)
        for x, at in ((near, heads(along, 2)), (over, heads(cross, 4)), (far, far_heads)):
            parts[c] += [x, send(x, pairs(at, 1))]
    for c in range(count - LAG, count):
        finish(c)
    return caches[0], caches[1], out


def local_step(c_raw, k_raw, norm_gain, rope_cos, rope_sin, seq_lens, q_lat, q_rope):
    me = lax.axis_index("x")
    left = count_units(seq_lens)
    need = jnp.sum((left > 0).astype(jnp.int32), axis=-1)
    fits = []
    for plan in PLANS:
        cap = np.stack([[plan.cap[s, (s // 2) ^ chip] for chip in range(CHIPS)] for s in range(N)])
        fits.append(jnp.all(need <= jnp.asarray(cap)))
    which = jnp.argmax(jnp.stack(fits)).astype(jnp.int32)
    args = (me, left, c_raw, jnp.swapaxes(k_raw, 1, 2), norm_gain[None, :], rope_cos.T, rope_sin.T, q_lat, jnp.swapaxes(q_rope, 1, 2))
    branches = [lambda *a, plan=plan: run_plan(plan, *a) for plan in PLANS]
    c_cache, k_cache_t, o_lat = lax.switch(which, branches, *args) if len(PLANS) > 1 else branches[0](*args)
    return c_cache, jnp.swapaxes(k_cache_t, 1, 2), o_lat


def solution(mesh):
    seq_spec = P("dp", "x", None)
    req_spec = P(("dp", "x"), None, None)
    return jax.shard_map(
        local_step,
        mesh=mesh,
        in_specs=(seq_spec, seq_spec, P(None), P("x", None), P("x", None), P("dp"), req_spec, req_spec),
        out_specs=(req_spec, req_spec, req_spec),
        check_vma=False,
    )
```

```python
import jax
import jax.numpy as jnp
import numpy as np
from jax import lax
from jax.experimental import pallas as pl
from jax.experimental.pallas import tpu as pltpu
from jax.sharding import PartitionSpec as P

NORM_EPS = 1e-6
N = 8
CHIPS = 4
REQ = 12
SEQ = 768
RANK = 512
ROPE = 64
HEADS = 128
UNIT = 256
PER = SEQ // UNIT
PIECES = RANK // 128
HALVES = UNIT // 128
ROWS = PIECES * UNIT + HALVES * ROPE
SLOTS = 2 * REQ * PER
NONE = 10**6
ATTN_SCALE = (RANK + ROPE) ** -0.5
DEPTH = 2
LAG = 4


class Plan:
    def __init__(self, chunks):
        self.chunks = chunks
        self.starts = np.cumsum([0] + [c[0] for c in chunks])[:-1]
        assert sum(c[0] for c in chunks) == SLOTS
        self.slot = np.full((N, CHIPS, SLOTS), NONE, np.int32)
        self.cap = np.zeros((N, CHIPS), np.int32)
        for s in range(N):
            for q in range(CHIPS):
                for chunk, start in zip(chunks, self.starts):
                    width = chunk[0]
                    if q == 0 or s in chunk[q + 1]:
                        self.slot[s, q, start : start + width] = self.cap[s, q] + np.arange(width)
                        self.cap[s, q] += width


ALL = (0, 1, 2, 3, 4, 5, 6, 7)
UP = (0, 1, 2, 3)
LOW = (4, 5, 6, 7)


NO_CHIP1 = (0, 1, 4, 5, 6, 7)
NO_3 = (0, 1, 2, 4, 5, 6, 7)


def direct(width):
    return width, "direct", ALL, ALL, ALL


def relay(width):
    return width, "relay", UP, ALL, UP


def no_chip1(width):
    return width, "direct", ALL, NO_CHIP1, NO_CHIP1


def no_3(width):
    return width, "direct", ALL, NO_3, NO_3


def end(width):
    return width, "direct", UP, ALL, UP


PLANS = (
    Plan([direct(4), direct(8), relay(7), no_chip1(5), relay(7), no_chip1(5), no_3(6)] + [direct(8)] * 3 + [end(4), end(2)]),
    Plan([direct(4), direct(8), relay(6), no_chip1(6), relay(4), no_3(6)] + [direct(8)] * 4 + [end(4), end(2)]),
    Plan([direct(4)] + [direct(8)] * 8 + [direct(4)]),
)


def norm_pack(width, start, tabs, c_raw, k_t, gain, cos_t, sin_t, after):
    steps = CHIPS * width

    def kernel(req_ref, unit_ref, ok_ref, c_ref, k_ref, g_ref, cos_ref, sin_ref, *refs):
        outs, (buf, sem) = refs[len(after) : len(after) + CHIPS], refs[-2:]
        n = pl.program_id(0)
        q, j = n // width, n % width
        ok_at = lambda m: ok_ref[m // width * SLOTS + start + m % width] > 0
        drain = lambda m: pltpu.make_async_copy(buf.at[m % 2], outs[0].at[0], sem.at[m % 2]).wait()
        slot = n % 2

        @pl.when((n >= 2) & ok_at(jnp.maximum(n - 2, 0)))
        def _():
            drain(n)

        @pl.when(ok_at(n))
        def _():
            key = k_ref[0].astype(jnp.float32)
            lo, hi = key[: ROPE // 2], key[ROPE // 2 :]
            cos, sin = cos_ref[...], sin_ref[...]
            rot = jnp.concatenate([lo * cos - hi * sin, hi * cos + lo * sin], axis=0).astype(jnp.bfloat16)
            for p in range(HALVES):
                at = PIECES * UNIT + p * ROPE
                buf[slot, at : at + ROPE, :] = rot[:, p * 128 : (p + 1) * 128]
                x = c_ref[0, p * 128 : (p + 1) * 128, :].astype(jnp.float32)
                inv = lax.rsqrt(jnp.mean(x * x, axis=-1, keepdims=True) + NORM_EPS)
                y = (x * inv * g_ref[...].astype(jnp.float32)).astype(jnp.bfloat16)
                for i in range(PIECES):
                    at = i * UNIT + p * 128
                    buf[slot, at : at + 128, :] = y[:, i * 128 : (i + 1) * 128]
            for mine in range(CHIPS):

                @pl.when(q == mine)
                def _(mine=mine):
                    pltpu.make_async_copy(buf.at[slot], outs[mine].at[j], sem.at[slot]).start()

        @pl.when(n == steps - 1)
        def _():
            @pl.when(ok_at(n - 1))
            def _():
                drain(n - 1)

            @pl.when(ok_at(n))
            def _():
                drain(n)

    def at(n):
        return n // width * SLOTS + start + n % width

    grid_spec = pltpu.PrefetchScalarGridSpec(
        num_scalar_prefetch=3,
        grid=(steps,),
        in_specs=[
            pl.BlockSpec((1, UNIT, RANK), lambda n, req, unit, ok: (req[at(n)], unit[at(n)], 0)),
            pl.BlockSpec((1, ROPE, UNIT), lambda n, req, unit, ok: (req[at(n)], 0, unit[at(n)])),
            pl.BlockSpec((1, RANK), lambda n, *_: (0, 0)),
            pl.BlockSpec((ROPE // 2, UNIT), lambda n, req, unit, ok: (0, unit[at(n)])),
            pl.BlockSpec((ROPE // 2, UNIT), lambda n, req, unit, ok: (0, unit[at(n)])),
        ]
        + [pl.BlockSpec(memory_space=pl.ANY)] * len(after),
        out_specs=[pl.BlockSpec(memory_space=pl.ANY)] * CHIPS,
        scratch_shapes=[pltpu.VMEM((2, ROWS, 128), jnp.bfloat16), pltpu.SemaphoreType.DMA((2,))],
    )
    return pl.pallas_call(
        kernel,
        grid_spec=grid_spec,
        out_shape=[jax.ShapeDtypeStruct((width, ROWS, 128), jnp.bfloat16)] * CHIPS,
        cost_estimate=pl.CostEstimate(flops=width * 10**8, bytes_accessed=width * 4 * 589824, transcendentals=0),
        name="norm_pack",
    )(*tabs, c_raw, k_t, gain, cos_t, sin_t, *after)


def attend(chunk, start, first, last, counts, codes, parts, q_lat, q_rope_t, caches, state):
    def kernel(count_ref, code_ref, *refs):
        part_refs, (qa_ref, qr_ref) = refs[:N], refs[N : N + 2]
        old_ref = None if first else refs[N + 4]
        outs = refs[N + (4 if first else 5) :]
        c_out, k_out, st_ref = outs[:3]
        buf, c_buf, k_buf, in_sem, c_sem, k_sem = outs[-6:]
        steps = count_ref[chunk]

        def fetch(n):
            code = code_ref[N * start + n]
            part, place = code // 2**22, code // 2**18 % 16
            for k in range(N):

                @pl.when(part == k)
                def _(k=k):
                    pltpu.make_async_copy(part_refs[k].at[place], buf.at[n % 3], in_sem.at[n % 3]).start()

        def drain(slot):
            pltpu.make_async_copy(c_buf.at[slot], c_out.at[0, pl.ds(0, UNIT), :], c_sem.at[slot]).wait()
            pltpu.make_async_copy(k_buf.at[slot], k_out.at[0, :, pl.ds(0, UNIT)], k_sem.at[slot]).wait()

        def step(n, _):
            code = code_ref[N * start + n]
            left, r = code // 2**9 % 2**9, code // 2**5 % 16
            at = pl.ds(pl.multiple_of(code % 2**5 * UNIT, UNIT), UNIT)
            slot = n % 2

            @pl.when(n + 2 < steps)
            def _():
                fetch(n + 2)

            pltpu.make_async_copy(part_refs[0].at[0], buf.at[n % 3], in_sem.at[n % 3]).wait()

            @pl.when(n >= 2)
            def _():
                drain(slot)

            row_ok = lax.broadcasted_iota(jnp.int32, (UNIT, 1), 0) < left
            lane_ok = lax.broadcasted_iota(jnp.int32, (1, UNIT), 1) < left
            for i in range(PIECES):
                piece = jnp.where(row_ok, buf[n % 3, i * UNIT : (i + 1) * UNIT, :].astype(jnp.float32), 0.0)
                c_buf[slot, :, i * 128 : (i + 1) * 128] = piece.astype(jnp.bfloat16)
            for p in range(HALVES):
                base = PIECES * UNIT + p * ROPE
                key = buf[n % 3, base : base + ROPE, :].astype(jnp.float32)
                key = jnp.where(lane_ok[:, p * 128 : (p + 1) * 128], key, 0.0)
                k_buf[slot, :, p * 128 : (p + 1) * 128] = key.astype(jnp.bfloat16)
            pltpu.make_async_copy(c_buf.at[slot], c_out.at[r, at, :], c_sem.at[slot]).start()
            pltpu.make_async_copy(k_buf.at[slot], k_out.at[r, :, at], k_sem.at[slot]).start()

            c = c_buf[slot]
            scores = lax.dot_general(qa_ref[r], c, (((1,), (1,)), ((), ())), preferred_element_type=jnp.float32)
            scores += lax.dot_general(qr_ref[r], k_buf[slot], (((0,), (0,)), ((), ())), preferred_element_type=jnp.float32)
            scores = jnp.where(lane_ok, scores * ATTN_SCALE, -1e30)
            l_old = st_ref[r, :, RANK : RANK + 1]
            m_old = st_ref[r, :, RANK + 128 : RANK + 129]
            m_new = jnp.maximum(m_old, jnp.max(scores, axis=-1, keepdims=True))
            weights = jnp.exp(scores - m_new)
            decay = jnp.exp(m_old - m_new)
            l_new = l_old * decay + jnp.sum(weights, axis=-1, keepdims=True)
            st_ref[r, :, RANK : RANK + 128] = jnp.broadcast_to(l_new, (HEADS, 128))
            st_ref[r, :, RANK + 128 :] = jnp.broadcast_to(m_new, (HEADS, 128))
            st_ref[r, :, :RANK] = st_ref[r, :, :RANK] * decay + jnp.dot(
                weights.astype(jnp.bfloat16), c, preferred_element_type=jnp.float32
            )
            return 0

        @pl.when(steps > 0)
        def _():
            fetch(0)

        @pl.when(steps > 1)
        def _():
            fetch(1)

        if first:
            st_ref[:, :, : RANK + 128] = jnp.zeros((REQ, HEADS, RANK + 128), jnp.float32)
            st_ref[:, :, RANK + 128 :] = jnp.full((REQ, HEADS, 128), -1e30, jnp.float32)
        else:
            st_ref[...] = old_ref[...]
        lax.fori_loop(0, steps, step, 0)

        @pl.when(steps > 1)
        def _():
            drain(steps % 2)

        @pl.when(steps > 0)
        def _():
            drain((steps + 1) % 2)

        if last:
            o_ref = outs[3]

            def finish(r, _):
                o_ref[r] = (st_ref[r, :, :RANK] / st_ref[r, :, RANK : RANK + 1]).astype(jnp.bfloat16)
                return 0

            lax.fori_loop(0, REQ, finish, 0)

    smem, vmem, anywhere = (pl.BlockSpec(memory_space=m) for m in (pltpu.SMEM, pltpu.VMEM, pl.ANY))
    state_shape = (REQ, HEADS, RANK + 256)
    in_specs = [smem] * 2 + [anywhere] * N + [vmem] * 2 + [anywhere] * 2
    operands = [counts, codes, *parts, q_lat, q_rope_t]
    aliases = {len(operands): 0, len(operands) + 1: 1}
    operands += list(caches)
    if not first:
        in_specs.append(vmem)
        operands.append(state)
    out_specs = [anywhere, anywhere, vmem]
    out_shape = [jax.ShapeDtypeStruct(c.shape, c.dtype) for c in caches] + [jax.ShapeDtypeStruct(state_shape, jnp.float32)]
    if last:
        out_specs.append(vmem)
        out_shape.append(jax.ShapeDtypeStruct((REQ, HEADS, RANK), jnp.bfloat16))
    return pl.pallas_call(
        kernel,
        in_specs=in_specs,
        out_specs=out_specs,
        out_shape=out_shape,
        scratch_shapes=[
            pltpu.VMEM((3, ROWS, 128), jnp.bfloat16),
            pltpu.VMEM((2, UNIT, RANK), jnp.bfloat16),
            pltpu.VMEM((2, ROPE, UNIT), jnp.bfloat16),
            pltpu.SemaphoreType.DMA((3,)),
            pltpu.SemaphoreType.DMA((2,)),
            pltpu.SemaphoreType.DMA((2,)),
        ],
        input_output_aliases=aliases,
        cost_estimate=pl.CostEstimate(flops=2 * 10**8, bytes_accessed=8 * 589824, transcendentals=0),
        name="attend",
    )(*operands)


def blank_caches(lens):
    def kernel(len_ref, c_ref, k_ref, c_zero, k_zero, c_sem, k_sem):
        c_zero[...] = jnp.zeros_like(c_zero)
        k_zero[...] = jnp.zeros_like(k_zero)

        def each(act):
            def block(n, _):
                r, s = n // N, n % N

                @pl.when(len_ref[r] < (s + 1) * SEQ)
                def _():
                    at = pl.ds(pl.multiple_of(s * SEQ, SEQ), SEQ)
                    act(pltpu.make_async_copy(c_zero, c_ref.at[r, at, :], c_sem.at[n]))
                    act(pltpu.make_async_copy(k_zero, k_ref.at[r, :, at], k_sem.at[n]))

                return 0

            lax.fori_loop(0, REQ * N, block, 0)

        each(lambda copy: copy.start())
        each(lambda copy: copy.wait())

    return pl.pallas_call(
        kernel,
        in_specs=[pl.BlockSpec(memory_space=pltpu.SMEM)],
        out_specs=[pl.BlockSpec(memory_space=pl.ANY)] * 2,
        out_shape=[
            jax.ShapeDtypeStruct((REQ, N * SEQ, RANK), jnp.bfloat16),
            jax.ShapeDtypeStruct((REQ, ROPE, N * SEQ), jnp.bfloat16),
        ],
        scratch_shapes=[
            pltpu.VMEM((SEQ, RANK), jnp.bfloat16),
            pltpu.VMEM((ROPE, SEQ), jnp.bfloat16),
            pltpu.SemaphoreType.DMA((REQ * N,)),
            pltpu.SemaphoreType.DMA((REQ * N,)),
        ],
        cost_estimate=pl.CostEstimate(flops=4 * 10**8, bytes_accessed=85 * 10**6, transcendentals=0),
        name="blank",
    )(lens)


def count_units(seq_lens):
    valid = jnp.clip(seq_lens[None, :] - SEQ * jnp.arange(N, dtype=jnp.int32)[:, None], 0, SEQ)
    left = valid.reshape(N, CHIPS, 2, REQ)[..., None] - UNIT * jnp.arange(PER, dtype=jnp.int32)
    left = left.transpose(0, 1, 3, 4, 2).reshape(N, CHIPS, SLOTS)
    return left


def split_place(place):
    return place // (2 * PER), place // 2 % PER, place % 2


def run_plan(plan, me, left, own_lens, c_raw, k_t, gain, cos_t, sin_t, q_lat, q_rope_t):
    chip = me // 2
    have = left > 0
    rank = jnp.cumsum(have.astype(jnp.int32), axis=-1)
    places = jnp.arange(SLOTS, dtype=jnp.int32)

    chips = chip ^ jnp.arange(CHIPS)
    mine = rank[me][chips]
    slot = jnp.asarray(plan.slot)[me]
    place = jnp.sum((mine[:, None, :] <= slot[:, :, None]).astype(jnp.int32), axis=-1)
    final = jnp.max(jnp.where(have[me][chips], places, 0), axis=-1, keepdims=True)
    held = jnp.minimum(place, final)
    req, unit, core = split_place(held)
    pack_tabs = [
        ((2 * chips[:, None] + core) * REQ + req).reshape(-1),
        unit.reshape(-1),
        (place < SLOTS).astype(jnp.int32).reshape(-1),
    ]

    part = jnp.arange(N)
    source = me ^ part
    theirs = rank[source, chip]
    slot = jnp.asarray(plan.slot)[source, part // 2]
    place = jnp.sum((theirs[:, None, :] <= slot[:, :, None]).astype(jnp.int32), axis=-1)
    req, unit, core = split_place(place)
    rows = jnp.sum(jnp.where(place[:, :, None] == places, left[source, chip][:, None, :], 0), axis=-1)
    rows = jnp.where(core == me % 2, jnp.minimum(rows, UNIT), 0)
    code = part[:, None] * 2**22 + rows * 2**9 + req * 2**5 + source[:, None] * PER + unit
    inside = np.concatenate([np.arange(c[0]) for c in plan.chunks]).astype(np.int32)
    code = jnp.where(rows > 0, code + jnp.asarray(inside) * 2**18, 0)
    code = jnp.concatenate([code[:, s : s + c[0]].reshape(-1) for c, s in zip(plan.chunks, plan.starts)])
    chunk_of = np.repeat(np.arange(len(plan.chunks)), [N * c[0] for c in plan.chunks])
    heads = (N * plan.starts)[chunk_of].astype(np.int32)
    same = jnp.asarray(chunk_of.astype(np.int32))[:, None] == jnp.asarray(chunk_of.astype(np.int32))[None, :]
    number = jnp.arange(N * SLOTS, dtype=jnp.int32)
    before = jnp.sum((same & (number[None, :] < number[:, None]) & (code > 0)[None, :]).astype(jnp.int32), axis=-1)
    goes_to = jnp.where(code > 0, jnp.asarray(heads) + before, -1)
    codes = jnp.sum(jnp.where(goes_to[None, :] == number[:, None], code[None, :], 0), axis=-1)
    in_chunk = jnp.asarray(chunk_of.astype(np.int32))[None, :] == jnp.arange(len(plan.chunks), dtype=jnp.int32)[:, None]
    counts = jnp.sum((in_chunk & (code > 0)[None, :]).astype(jnp.int32), axis=-1)

    pairs = lambda sources, hop: [(s, s ^ hop) for s in sources]
    send = lambda x, pairs: lax.ppermute(x, "x", pairs)
    caches = blank_caches(own_lens)
    state = out = None
    landed, parts, done = [], [], []
    count = len(plan.chunks)

    def finish(c):
        nonlocal caches, state, out
        got = attend(c, int(plan.starts[c]), c == 0, c == count - 1, counts, codes, parts[c], q_lat, q_rope_t, caches, state)
        caches, state = got[:2], got[2]
        if c == count - 1:
            out = got[3]

    after = []
    for c, (width, kind, along, across, diagonal) in enumerate(plan.chunks):
        if c >= LAG:
            finish(c - LAG)
            after = after + [state]
        staged = norm_pack(width, int(plan.starts[c]), pack_tabs, c_raw, k_t, gain, cos_t, sin_t, after)
        after = [staged[0]]
        sends = list(staged)
        if c >= DEPTH:
            sends, landed[c - DEPTH] = lax.optimization_barrier((sends, landed[c - DEPTH]))
        own = sends[0]
        lower = [(t, t ^ 1) for t in LOW]
        far = send(sends[3], pairs(ALL, 4) if kind == "relay" else pairs(diagonal, 6))
        near = send(sends[1], pairs(UP, 2) + lower if along == UP else pairs(ALL, 2))
        over = send(sends[2], pairs(across, 4))
        landed.append([near, over, far])
        parts.append([own, send(own, pairs(ALL, 1))])
        if kind == "relay":
            far = send(far, pairs(LOW, 2) + [(t, t ^ 1) for t in UP])
        for x in (near, over, far):
            parts[c] += [x, send(x, pairs(ALL, 1))]
    for c in range(count - LAG, count):
        finish(c)
    return caches[0], caches[1], out


def local_step(c_raw, k_raw, norm_gain, rope_cos, rope_sin, seq_lens, q_lat, q_rope):
    me = lax.axis_index("x")
    left = count_units(seq_lens)
    need = jnp.sum((left > 0).astype(jnp.int32), axis=-1)
    fits = []
    for plan in PLANS:
        cap = np.stack([[plan.cap[s, (s // 2) ^ chip] for chip in range(CHIPS)] for s in range(N)])
        fits.append(jnp.all(need <= jnp.asarray(cap)))
    which = jnp.argmax(jnp.stack(fits)).astype(jnp.int32)
    own_lens = lax.dynamic_slice_in_dim(seq_lens, me * REQ, REQ)
    args = (me, left, own_lens, c_raw, jnp.swapaxes(k_raw, 1, 2), norm_gain[None, :], rope_cos.T, rope_sin.T, q_lat, jnp.swapaxes(q_rope, 1, 2))
    branches = [lambda *a, plan=plan: run_plan(plan, *a) for plan in PLANS]
    c_cache, k_cache_t, o_lat = lax.switch(which, branches, *args) if len(PLANS) > 1 else branches[0](*args)
    return c_cache, jnp.swapaxes(k_cache_t, 1, 2), o_lat


def solution(mesh):
    seq_spec = P("dp", "x", None)
    req_spec = P(("dp", "x"), None, None)
    return jax.shard_map(
        local_step,
        mesh=mesh,
        in_specs=(seq_spec, seq_spec, P(None), P("x", None), P("x", None), P("dp"), req_spec, req_spec),
        out_specs=(req_spec, req_spec, req_spec),
        check_vma=False,
    )
```

```python
import functools

import jax
import jax.numpy as jnp
import numpy as np
from jax import lax
from jax.experimental import pallas as pl
from jax.experimental.pallas import tpu as pltpu
from jax.sharding import PartitionSpec as P

NORM_EPS = 1e-6
N = 8
CHIPS = 4
REQ = 12
SEQ = 768
RANK = 512
ROPE = 64
HEADS = 128
UNIT = 256
PER = SEQ // UNIT
PIECES = RANK // 128
HALVES = UNIT // 128
ROWS = PIECES * UNIT + HALVES * ROPE
SLOTS = 2 * REQ * PER
NONE = 10**6
ATTN_SCALE = (RANK + ROPE) ** -0.5
DEPTH = 2


class Plan:
    def __init__(self, chunks):
        self.chunks = chunks
        self.starts = np.cumsum([0] + [c[0] for c in chunks])[:-1]
        assert sum(c[0] for c in chunks) == SLOTS
        self.slot = np.full((N, CHIPS, SLOTS), NONE, np.int32)
        self.cap = np.zeros((N, CHIPS), np.int32)
        for s in range(N):
            for q in range(CHIPS):
                for chunk, start in zip(chunks, self.starts):
                    width = chunk[0]
                    if q == 0 or s in chunk[q + 1]:
                        self.slot[s, q, start : start + width] = self.cap[s, q] + np.arange(width)
                        self.cap[s, q] += width


ALL = (0, 1, 2, 3, 4, 5, 6, 7)
UP = (0, 1, 2, 3)
LOW = (4, 5, 6, 7)


NO_CHIP1 = (0, 1, 4, 5, 6, 7)
NO_3 = (0, 1, 2, 4, 5, 6, 7)


def direct(width):
    return width, "direct", ALL, ALL, ALL


def relay(width):
    return width, "relay", UP, ALL, UP


def no_chip1(width):
    return width, "direct", ALL, NO_CHIP1, NO_CHIP1


def no_3(width):
    return width, "direct", ALL, NO_3, NO_3


def end(width):
    return width, "direct", UP, ALL, UP


PLANS = (
    Plan([direct(4), direct(8), relay(7), no_chip1(5), relay(7), no_chip1(5), no_3(6)] + [direct(8)] * 3 + [end(4), end(2)]),
    Plan([direct(4), direct(8), relay(6), no_chip1(6), relay(4), no_3(6)] + [direct(8)] * 4 + [end(4), end(2)]),
    Plan([direct(4)] + [direct(8)] * 8 + [direct(4)]),
)


def norm_pack(width, start, tabs, c_raw, k_t, gain, cos_t, sin_t, after):
    steps = CHIPS * width

    def kernel(req_ref, unit_ref, ok_ref, c_ref, k_ref, g_ref, cos_ref, sin_ref, *refs):
        outs, (buf, sem) = refs[len(after) : len(after) + CHIPS], refs[-2:]
        n = pl.program_id(0)
        q, j = n // width, n % width
        ok_at = lambda m: ok_ref[m // width * SLOTS + start + m % width] > 0
        drain = lambda m: pltpu.make_async_copy(buf.at[m % 2], outs[0].at[0], sem.at[m % 2]).wait()
        slot = n % 2

        @pl.when((n >= 2) & ok_at(jnp.maximum(n - 2, 0)))
        def _():
            drain(n)

        @pl.when(ok_at(n))
        def _():
            key = k_ref[0].astype(jnp.float32)
            lo, hi = key[: ROPE // 2], key[ROPE // 2 :]
            cos, sin = cos_ref[...], sin_ref[...]
            rot = jnp.concatenate([lo * cos - hi * sin, hi * cos + lo * sin], axis=0).astype(jnp.bfloat16)
            for p in range(HALVES):
                at = PIECES * UNIT + p * ROPE
                buf[slot, at : at + ROPE, :] = rot[:, p * 128 : (p + 1) * 128]
                x = c_ref[0, p * 128 : (p + 1) * 128, :].astype(jnp.float32)
                inv = lax.rsqrt(jnp.mean(x * x, axis=-1, keepdims=True) + NORM_EPS)
                y = (x * inv * g_ref[...].astype(jnp.float32)).astype(jnp.bfloat16)
                for i in range(PIECES):
                    at = i * UNIT + p * 128
                    buf[slot, at : at + 128, :] = y[:, i * 128 : (i + 1) * 128]
            for mine in range(CHIPS):

                @pl.when(q == mine)
                def _(mine=mine):
                    pltpu.make_async_copy(buf.at[slot], outs[mine].at[j], sem.at[slot]).start()

        @pl.when(n == steps - 1)
        def _():
            @pl.when(ok_at(n - 1))
            def _():
                drain(n - 1)

            @pl.when(ok_at(n))
            def _():
                drain(n)

    def at(n):
        return n // width * SLOTS + start + n % width

    grid_spec = pltpu.PrefetchScalarGridSpec(
        num_scalar_prefetch=3,
        grid=(steps,),
        in_specs=[
            pl.BlockSpec((1, UNIT, RANK), lambda n, req, unit, ok: (req[at(n)], unit[at(n)], 0)),
            pl.BlockSpec((1, ROPE, UNIT), lambda n, req, unit, ok: (req[at(n)], 0, unit[at(n)])),
            pl.BlockSpec((1, RANK), lambda n, *_: (0, 0)),
            pl.BlockSpec((ROPE // 2, UNIT), lambda n, req, unit, ok: (0, unit[at(n)])),
            pl.BlockSpec((ROPE // 2, UNIT), lambda n, req, unit, ok: (0, unit[at(n)])),
        ]
        + [pl.BlockSpec(memory_space=pl.ANY)] * len(after),
        out_specs=[pl.BlockSpec(memory_space=pl.ANY)] * CHIPS,
        scratch_shapes=[pltpu.VMEM((2, ROWS, 128), jnp.bfloat16), pltpu.SemaphoreType.DMA((2,))],
    )
    return pl.pallas_call(
        kernel,
        grid_spec=grid_spec,
        out_shape=[jax.ShapeDtypeStruct((width, ROWS, 128), jnp.bfloat16)] * CHIPS,
        cost_estimate=pl.CostEstimate(flops=width * 10**8, bytes_accessed=width * 4 * 589824, transcendentals=0),
        name="norm_pack",
    )(*tabs, c_raw, k_t, gain, cos_t, sin_t, *after)


def attend(chunk, start, first, last, counts, codes, parts, q_lat, q_rope_t, caches, state):
    def kernel(count_ref, code_ref, *refs):
        part_refs, (qa_ref, qr_ref) = refs[:N], refs[N : N + 2]
        old_ref = None if first else refs[N + 4]
        outs = refs[N + (4 if first else 5) :]
        c_out, k_out, st_ref = outs[:3]
        buf, c_buf, k_buf, in_sem, c_sem, k_sem = outs[-6:]
        steps = count_ref[chunk]

        def fetch(n):
            code = code_ref[N * start + n]
            part, place = code // 2**22, code // 2**18 % 16
            for k in range(N):

                @pl.when(part == k)
                def _(k=k):
                    pltpu.make_async_copy(part_refs[k].at[place], buf.at[n % 3], in_sem.at[n % 3]).start()

        def drain(slot):
            pltpu.make_async_copy(c_buf.at[slot], c_out.at[0, pl.ds(0, UNIT), :], c_sem.at[slot]).wait()
            pltpu.make_async_copy(k_buf.at[slot], k_out.at[0, :, pl.ds(0, UNIT)], k_sem.at[slot]).wait()

        def step(n, _):
            code = code_ref[N * start + n]
            left, r = code // 2**9 % 2**9, code // 2**5 % 16
            at = pl.ds(pl.multiple_of(code % 2**5 * UNIT, UNIT), UNIT)
            slot = n % 2

            @pl.when(n + 2 < steps)
            def _():
                fetch(n + 2)

            pltpu.make_async_copy(part_refs[0].at[0], buf.at[n % 3], in_sem.at[n % 3]).wait()

            @pl.when(n >= 2)
            def _():
                drain(slot)

            row_ok = lax.broadcasted_iota(jnp.int32, (UNIT, 1), 0) < left
            lane_ok = lax.broadcasted_iota(jnp.int32, (1, UNIT), 1) < left
            for i in range(PIECES):
                piece = jnp.where(row_ok, buf[n % 3, i * UNIT : (i + 1) * UNIT, :].astype(jnp.float32), 0.0)
                c_buf[slot, :, i * 128 : (i + 1) * 128] = piece.astype(jnp.bfloat16)
            for p in range(HALVES):
                base = PIECES * UNIT + p * ROPE
                key = buf[n % 3, base : base + ROPE, :].astype(jnp.float32)
                key = jnp.where(lane_ok[:, p * 128 : (p + 1) * 128], key, 0.0)
                k_buf[slot, :, p * 128 : (p + 1) * 128] = key.astype(jnp.bfloat16)
            pltpu.make_async_copy(c_buf.at[slot], c_out.at[r, at, :], c_sem.at[slot]).start()
            pltpu.make_async_copy(k_buf.at[slot], k_out.at[r, :, at], k_sem.at[slot]).start()

            c = c_buf[slot]
            scores = lax.dot_general(qa_ref[r], c, (((1,), (1,)), ((), ())), preferred_element_type=jnp.float32)
            scores += lax.dot_general(qr_ref[r], k_buf[slot], (((0,), (0,)), ((), ())), preferred_element_type=jnp.float32)
            scores = jnp.where(lane_ok, scores * ATTN_SCALE, -1e30)
            l_old = st_ref[r, :, RANK : RANK + 1]
            m_old = st_ref[r, :, RANK + 128 : RANK + 129]
            m_new = jnp.maximum(m_old, jnp.max(scores, axis=-1, keepdims=True))
            weights = jnp.exp(scores - m_new)
            decay = jnp.exp(m_old - m_new)
            l_new = l_old * decay + jnp.sum(weights, axis=-1, keepdims=True)
            st_ref[r, :, RANK : RANK + 128] = jnp.broadcast_to(l_new, (HEADS, 128))
            st_ref[r, :, RANK + 128 :] = jnp.broadcast_to(m_new, (HEADS, 128))
            st_ref[r, :, :RANK] = st_ref[r, :, :RANK] * decay + jnp.dot(
                weights.astype(jnp.bfloat16), c, preferred_element_type=jnp.float32
            )
            return 0

        @pl.when(steps > 0)
        def _():
            fetch(0)

        @pl.when(steps > 1)
        def _():
            fetch(1)

        if first:
            st_ref[:, :, : RANK + 128] = jnp.zeros((REQ, HEADS, RANK + 128), jnp.float32)
            st_ref[:, :, RANK + 128 :] = jnp.full((REQ, HEADS, 128), -1e30, jnp.float32)
        else:
            st_ref[...] = old_ref[...]
        lax.fori_loop(0, steps, step, 0)

        @pl.when(steps > 1)
        def _():
            drain(steps % 2)

        @pl.when(steps > 0)
        def _():
            drain((steps + 1) % 2)

        if last:
            o_ref = outs[3]

            def finish(r, _):
                o_ref[r] = (st_ref[r, :, :RANK] / st_ref[r, :, RANK : RANK + 1]).astype(jnp.bfloat16)
                return 0

            lax.fori_loop(0, REQ, finish, 0)

    smem, vmem, anywhere = (pl.BlockSpec(memory_space=m) for m in (pltpu.SMEM, pltpu.VMEM, pl.ANY))
    state_shape = (REQ, HEADS, RANK + 256)
    in_specs = [smem] * 2 + [anywhere] * N + [vmem] * 2 + [anywhere] * 2
    operands = [counts, codes, *parts, q_lat, q_rope_t]
    aliases = {len(operands): 0, len(operands) + 1: 1}
    operands += list(caches)
    if not first:
        in_specs.append(vmem)
        operands.append(state)
    out_specs = [anywhere, anywhere, vmem]
    out_shape = [jax.ShapeDtypeStruct(c.shape, c.dtype) for c in caches] + [jax.ShapeDtypeStruct(state_shape, jnp.float32)]
    if last:
        out_specs.append(vmem)
        out_shape.append(jax.ShapeDtypeStruct((REQ, HEADS, RANK), jnp.bfloat16))
    return pl.pallas_call(
        kernel,
        in_specs=in_specs,
        out_specs=out_specs,
        out_shape=out_shape,
        scratch_shapes=[
            pltpu.VMEM((3, ROWS, 128), jnp.bfloat16),
            pltpu.VMEM((2, UNIT, RANK), jnp.bfloat16),
            pltpu.VMEM((2, ROPE, UNIT), jnp.bfloat16),
            pltpu.SemaphoreType.DMA((3,)),
            pltpu.SemaphoreType.DMA((2,)),
            pltpu.SemaphoreType.DMA((2,)),
        ],
        input_output_aliases=aliases,
        cost_estimate=pl.CostEstimate(flops=2 * 10**8, bytes_accessed=8 * 589824, transcendentals=0),
        name="attend",
    )(*operands)


def blank_caches(lens):
    def kernel(len_ref, c_ref, k_ref, c_zero, k_zero, c_sem, k_sem):
        c_zero[...] = jnp.zeros_like(c_zero)
        k_zero[...] = jnp.zeros_like(k_zero)

        def each(act):
            def block(n, _):
                r, s = n // N, n % N

                @pl.when(len_ref[r] < (s + 1) * SEQ)
                def _():
                    at = pl.ds(pl.multiple_of(s * SEQ, SEQ), SEQ)
                    act(pltpu.make_async_copy(c_zero, c_ref.at[r, at, :], c_sem.at[n]))
                    act(pltpu.make_async_copy(k_zero, k_ref.at[r, :, at], k_sem.at[n]))

                return 0

            lax.fori_loop(0, REQ * N, block, 0)

        each(lambda copy: copy.start())
        each(lambda copy: copy.wait())

    return pl.pallas_call(
        kernel,
        in_specs=[pl.BlockSpec(memory_space=pltpu.SMEM)],
        out_specs=[pl.BlockSpec(memory_space=pl.ANY)] * 2,
        out_shape=[
            jax.ShapeDtypeStruct((REQ, N * SEQ, RANK), jnp.bfloat16),
            jax.ShapeDtypeStruct((REQ, ROPE, N * SEQ), jnp.bfloat16),
        ],
        scratch_shapes=[
            pltpu.VMEM((SEQ, RANK), jnp.bfloat16),
            pltpu.VMEM((ROPE, SEQ), jnp.bfloat16),
            pltpu.SemaphoreType.DMA((REQ * N,)),
            pltpu.SemaphoreType.DMA((REQ * N,)),
        ],
        cost_estimate=pl.CostEstimate(flops=4 * 10**8, bytes_accessed=85 * 10**6, transcendentals=0),
        name="blank",
    )(lens)


def count_units(seq_lens):
    valid = jnp.clip(seq_lens[None, :] - SEQ * jnp.arange(N, dtype=jnp.int32)[:, None], 0, SEQ)
    left = valid.reshape(N, CHIPS, 2, REQ)[..., None] - UNIT * jnp.arange(PER, dtype=jnp.int32)
    left = left.transpose(0, 1, 3, 4, 2).reshape(N, CHIPS, SLOTS)
    return left


def split_place(place):
    return place // (2 * PER), place // 2 % PER, place % 2


def run_plan(plan, me, left, own_lens, c_raw, k_t, gain, cos_t, sin_t, q_lat, q_rope_t):
    chip = me // 2
    have = left > 0
    rank = jnp.cumsum(have.astype(jnp.int32), axis=-1)
    places = jnp.arange(SLOTS, dtype=jnp.int32)

    chips = chip ^ jnp.arange(CHIPS)
    mine = rank[me][chips]
    slot = jnp.asarray(plan.slot)[me]
    place = jnp.sum((mine[:, None, :] <= slot[:, :, None]).astype(jnp.int32), axis=-1)
    final = jnp.max(jnp.where(have[me][chips], places, 0), axis=-1, keepdims=True)
    held = jnp.minimum(place, final)
    req, unit, core = split_place(held)
    pack_tabs = [
        ((2 * chips[:, None] + core) * REQ + req).reshape(-1),
        unit.reshape(-1),
        (place < SLOTS).astype(jnp.int32).reshape(-1),
    ]

    part = jnp.arange(N)
    source = me ^ part
    theirs = rank[source, chip]
    slot = jnp.asarray(plan.slot)[source, part // 2]
    place = jnp.sum((theirs[:, None, :] <= slot[:, :, None]).astype(jnp.int32), axis=-1)
    req, unit, core = split_place(place)
    rows = jnp.sum(jnp.where(place[:, :, None] == places, left[source, chip][:, None, :], 0), axis=-1)
    rows = jnp.where(core == me % 2, jnp.minimum(rows, UNIT), 0)
    code = part[:, None] * 2**22 + rows * 2**9 + req * 2**5 + source[:, None] * PER + unit
    inside = np.concatenate([np.arange(c[0]) for c in plan.chunks]).astype(np.int32)
    code = jnp.where(rows > 0, code + jnp.asarray(inside) * 2**18, 0)
    code = jnp.concatenate([code[:, s : s + c[0]].reshape(-1) for c, s in zip(plan.chunks, plan.starts)])
    chunk_of = np.repeat(np.arange(len(plan.chunks)), [N * c[0] for c in plan.chunks])
    heads = (N * plan.starts)[chunk_of].astype(np.int32)
    same = jnp.asarray(chunk_of.astype(np.int32))[:, None] == jnp.asarray(chunk_of.astype(np.int32))[None, :]
    number = jnp.arange(N * SLOTS, dtype=jnp.int32)
    before = jnp.sum((same & (number[None, :] < number[:, None]) & (code > 0)[None, :]).astype(jnp.int32), axis=-1)
    goes_to = jnp.where(code > 0, jnp.asarray(heads) + before, -1)
    codes = jnp.sum(jnp.where(goes_to[None, :] == number[:, None], code[None, :], 0), axis=-1)
    in_chunk = jnp.asarray(chunk_of.astype(np.int32))[None, :] == jnp.arange(len(plan.chunks), dtype=jnp.int32)[:, None]
    counts = jnp.sum((in_chunk & (code > 0)[None, :]).astype(jnp.int32), axis=-1)

    pairs = lambda sources, hop: [(s, s ^ hop) for s in sources]

    def send(x, pairs):
        return lax.ppermute(x, "x", pairs)

    caches = blank_caches(own_lens)
    state = None
    landed, owns, twins = [], [], []
    count = len(plan.chunks)

    after = []
    for c, (width, kind, along, across, diagonal) in enumerate(plan.chunks):
        staged = norm_pack(width, int(plan.starts[c]), pack_tabs, c_raw, k_t, gain, cos_t, sin_t, after)
        after = [staged[0]]
        sends = list(staged)
        if c >= DEPTH:
            sends, landed[c - DEPTH] = lax.optimization_barrier((sends, landed[c - DEPTH]))
        owns.append(sends[0])
        twins.append(send(sends[0], pairs(ALL, 1)))
        lower = [(t, t ^ 1) for t in LOW]
        far = send(sends[3], pairs(ALL, 4) if kind == "relay" else pairs(diagonal, 6))
        near = send(sends[1], pairs(UP, 2) + lower if along == UP else pairs(ALL, 2))
        over = send(sends[2], pairs(across, 4))
        landed.append([near, over, far])
    for c, (_, kind, _, _, _) in enumerate(plan.chunks):
        near, over, far = landed[c]
        if kind == "relay":
            far = send(far, pairs(LOW, 2) + [(t, t ^ 1) for t in UP])
        parts = [owns[c], twins[c]]
        for x in (near, over, far):
            parts += [x, send(x, pairs(ALL, 1))]
        got = attend(c, int(plan.starts[c]), c == 0, c == count - 1, counts, codes, parts, q_lat, q_rope_t, caches, state)
        caches, state = got[:2], got[2]
    return caches[0], caches[1], got[3]


def local_step(c_raw, k_raw, norm_gain, rope_cos, rope_sin, seq_lens, q_lat, q_rope):
    me = lax.axis_index("x")
    left = count_units(seq_lens)
    need = jnp.sum((left > 0).astype(jnp.int32), axis=-1)
    fits = []
    for plan in PLANS:
        cap = np.stack([[plan.cap[s, (s // 2) ^ chip] for chip in range(CHIPS)] for s in range(N)])
        fits.append(jnp.all(need <= jnp.asarray(cap)))
    which = jnp.argmax(jnp.stack(fits)).astype(jnp.int32)
    own_lens = lax.dynamic_slice_in_dim(seq_lens, me * REQ, REQ)
    args = (me, left, own_lens, c_raw, jnp.swapaxes(k_raw, 1, 2), norm_gain[None, :], rope_cos.T, rope_sin.T, q_lat, jnp.swapaxes(q_rope, 1, 2))

    def branch(number, *args):
        return run_plan(PLANS[number], *args)

    branches = [functools.partial(branch, number) for number in range(len(PLANS))]
    c_cache, k_cache_t, o_lat = lax.switch(which, branches, *args) if len(PLANS) > 1 else branches[0](*args)
    return c_cache, jnp.swapaxes(k_cache_t, 1, 2), o_lat


def solution(mesh):
    seq_spec = P("dp", "x", None)
    req_spec = P(("dp", "x"), None, None)
    return jax.shard_map(
        local_step,
        mesh=mesh,
        in_specs=(seq_spec, seq_spec, P(None), P("x", None), P("x", None), P("dp"), req_spec, req_spec),
        out_specs=(req_spec, req_spec, req_spec),
        check_vma=False,
    )
```

```python
import jax
import jax.numpy as jnp
import numpy as np
from jax import lax
from jax.experimental import pallas as pl
from jax.experimental.pallas import tpu as pltpu
from jax.sharding import PartitionSpec as P

NORM_EPS = 1e-6
N = 8
CHIPS = 4
REQ = 12
SEQ = 768
RANK = 512
ROPE = 64
HEADS = 128
UNIT = 256
PER = SEQ // UNIT
PIECES = RANK // 128
HALVES = UNIT // 128
ROWS = PIECES * UNIT + HALVES * ROPE
SLOTS = 2 * REQ * PER
NONE = 10**6
ATTN_SCALE = (RANK + ROPE) ** -0.5
DEPTH = 2


class Plan:
    def __init__(self, chunks):
        self.chunks = chunks
        self.starts = np.cumsum([0] + [c[0] for c in chunks])[:-1]
        assert sum(c[0] for c in chunks) == SLOTS
        self.slot = np.full((N, CHIPS, SLOTS), NONE, np.int32)
        self.cap = np.zeros((N, CHIPS), np.int32)
        for s in range(N):
            for q in range(CHIPS):
                for chunk, start in zip(chunks, self.starts):
                    width = chunk[0]
                    if q == 0 or s in chunk[q + 1]:
                        self.slot[s, q, start : start + width] = self.cap[s, q] + np.arange(width)
                        self.cap[s, q] += width


ALL = (0, 1, 2, 3, 4, 5, 6, 7)
UP = (0, 1, 2, 3)
LOW = (4, 5, 6, 7)


NO_CHIP1 = (0, 1, 4, 5, 6, 7)
NO_3 = (0, 1, 2, 4, 5, 6, 7)


def direct(width):
    return width, "direct", ALL, ALL, ALL


def relay(width):
    return width, "relay", UP, ALL, UP


def no_chip1(width):
    return width, "direct", ALL, NO_CHIP1, NO_CHIP1


def no_3(width):
    return width, "direct", ALL, NO_3, NO_3


def end(width):
    return width, "direct", UP, ALL, UP


PLAN = Plan(
    [direct(2), direct(4), direct(6), relay(6), no_chip1(6), relay(4), no_3(6)] + [direct(8)] * 4 + [end(4), end(2)]
)
EXTRA = 4


def norm_pack(width, start, stride, tabs, c_raw, k_t, gain, cos_t, sin_t, after):
    steps = CHIPS * width

    def kernel(req_ref, unit_ref, ok_ref, c_ref, k_ref, g_ref, cos_ref, sin_ref, *refs):
        outs, (buf, sem) = refs[len(after) : len(after) + CHIPS], refs[-2:]
        n = pl.program_id(0)
        q, j = n // width, n % width
        ok_at = lambda m: ok_ref[m // width * stride + start + m % width] > 0
        drain = lambda m: pltpu.make_async_copy(buf.at[m % 2], outs[0].at[0], sem.at[m % 2]).wait()
        slot = n % 2

        @pl.when((n >= 2) & ok_at(jnp.maximum(n - 2, 0)))
        def _():
            drain(n)

        @pl.when(ok_at(n))
        def _():
            key = k_ref[0].astype(jnp.float32)
            lo, hi = key[: ROPE // 2], key[ROPE // 2 :]
            cos, sin = cos_ref[...], sin_ref[...]
            rot = jnp.concatenate([lo * cos - hi * sin, hi * cos + lo * sin], axis=0).astype(jnp.bfloat16)
            for p in range(HALVES):
                at = PIECES * UNIT + p * ROPE
                buf[slot, at : at + ROPE, :] = rot[:, p * 128 : (p + 1) * 128]
                x = c_ref[0, p * 128 : (p + 1) * 128, :].astype(jnp.float32)
                inv = lax.rsqrt(jnp.mean(x * x, axis=-1, keepdims=True) + NORM_EPS)
                y = (x * inv * g_ref[...].astype(jnp.float32)).astype(jnp.bfloat16)
                for i in range(PIECES):
                    at = i * UNIT + p * 128
                    buf[slot, at : at + 128, :] = y[:, i * 128 : (i + 1) * 128]
            for mine in range(CHIPS):

                @pl.when(q == mine)
                def _(mine=mine):
                    pltpu.make_async_copy(buf.at[slot], outs[mine].at[j], sem.at[slot]).start()

        @pl.when(n == steps - 1)
        def _():
            @pl.when(ok_at(n - 1))
            def _():
                drain(n - 1)

            @pl.when(ok_at(n))
            def _():
                drain(n)

    def at(n):
        return n // width * stride + start + n % width

    grid_spec = pltpu.PrefetchScalarGridSpec(
        num_scalar_prefetch=3,
        grid=(steps,),
        in_specs=[
            pl.BlockSpec((1, UNIT, RANK), lambda n, req, unit, ok: (req[at(n)], unit[at(n)], 0)),
            pl.BlockSpec((1, ROPE, UNIT), lambda n, req, unit, ok: (req[at(n)], 0, unit[at(n)])),
            pl.BlockSpec((1, RANK), lambda n, *_: (0, 0)),
            pl.BlockSpec((ROPE // 2, UNIT), lambda n, req, unit, ok: (0, unit[at(n)])),
            pl.BlockSpec((ROPE // 2, UNIT), lambda n, req, unit, ok: (0, unit[at(n)])),
        ]
        + [pl.BlockSpec(memory_space=pl.ANY)] * len(after),
        out_specs=[pl.BlockSpec(memory_space=pl.ANY)] * CHIPS,
        scratch_shapes=[pltpu.VMEM((2, ROWS, 128), jnp.bfloat16), pltpu.SemaphoreType.DMA((2,))],
    )
    return pl.pallas_call(
        kernel,
        grid_spec=grid_spec,
        out_shape=[jax.ShapeDtypeStruct((width, ROWS, 128), jnp.bfloat16)] * CHIPS,
        cost_estimate=pl.CostEstimate(flops=width * 10**8, bytes_accessed=width * 4 * 589824, transcendentals=0),
        name="norm_pack",
    )(*tabs, c_raw, k_t, gain, cos_t, sin_t, *after)


def attend(chunk, start, first, counts, codes, parts, q_lat, q_rope_t, caches, state):
    total = len(parts)

    def kernel(count_ref, code_ref, *refs):
        part_refs, (qa_ref, qr_ref) = refs[:total], refs[total : total + 2]
        old_ref = None if first else refs[total + 4]
        outs = refs[total + (4 if first else 5) :]
        c_out, k_out, st_ref = outs[:3]
        buf, c_buf, k_buf, in_sem, c_sem, k_sem = outs[-6:]
        steps = count_ref[chunk]

        def fetch(n):
            code = code_ref[start + n]
            part, place = code // 2**22, code // 2**18 % 16
            for k in range(total):

                @pl.when(part == k)
                def _(k=k):
                    pltpu.make_async_copy(part_refs[k].at[place], buf.at[n % 3], in_sem.at[n % 3]).start()

        def drain(slot):
            pltpu.make_async_copy(c_buf.at[slot], c_out.at[0, pl.ds(0, UNIT), :], c_sem.at[slot]).wait()
            pltpu.make_async_copy(k_buf.at[slot], k_out.at[0, :, pl.ds(0, UNIT)], k_sem.at[slot]).wait()

        def step(n, _):
            code = code_ref[start + n]
            left, r = code // 2**9 % 2**9, code // 2**5 % 16
            at = pl.ds(pl.multiple_of(code % 2**5 * UNIT, UNIT), UNIT)
            slot = n % 2

            @pl.when(n + 2 < steps)
            def _():
                fetch(n + 2)

            pltpu.make_async_copy(part_refs[0].at[0], buf.at[n % 3], in_sem.at[n % 3]).wait()

            @pl.when(n >= 2)
            def _():
                drain(slot)

            row_ok = lax.broadcasted_iota(jnp.int32, (UNIT, 1), 0) < left
            lane_ok = lax.broadcasted_iota(jnp.int32, (1, UNIT), 1) < left
            for i in range(PIECES):
                piece = jnp.where(row_ok, buf[n % 3, i * UNIT : (i + 1) * UNIT, :].astype(jnp.float32), 0.0)
                c_buf[slot, :, i * 128 : (i + 1) * 128] = piece.astype(jnp.bfloat16)
            for p in range(HALVES):
                base = PIECES * UNIT + p * ROPE
                key = buf[n % 3, base : base + ROPE, :].astype(jnp.float32)
                key = jnp.where(lane_ok[:, p * 128 : (p + 1) * 128], key, 0.0)
                k_buf[slot, :, p * 128 : (p + 1) * 128] = key.astype(jnp.bfloat16)
            pltpu.make_async_copy(c_buf.at[slot], c_out.at[r, at, :], c_sem.at[slot]).start()
            pltpu.make_async_copy(k_buf.at[slot], k_out.at[r, :, at], k_sem.at[slot]).start()

            c = c_buf[slot]
            scores = lax.dot_general(qa_ref[r], c, (((1,), (1,)), ((), ())), preferred_element_type=jnp.float32)
            scores += lax.dot_general(qr_ref[r], k_buf[slot], (((0,), (0,)), ((), ())), preferred_element_type=jnp.float32)
            scores = jnp.where(lane_ok, scores * ATTN_SCALE, -1e30)
            l_old = st_ref[r, :, RANK : RANK + 1]
            m_old = st_ref[r, :, RANK + 128 : RANK + 129]
            m_new = jnp.maximum(m_old, jnp.max(scores, axis=-1, keepdims=True))
            weights = jnp.exp(scores - m_new)
            decay = jnp.exp(m_old - m_new)
            l_new = l_old * decay + jnp.sum(weights, axis=-1, keepdims=True)
            st_ref[r, :, RANK : RANK + 128] = jnp.broadcast_to(l_new, (HEADS, 128))
            st_ref[r, :, RANK + 128 :] = jnp.broadcast_to(m_new, (HEADS, 128))
            st_ref[r, :, :RANK] = st_ref[r, :, :RANK] * decay + jnp.dot(
                weights.astype(jnp.bfloat16), c, preferred_element_type=jnp.float32
            )
            return 0

        @pl.when(steps > 0)
        def _():
            fetch(0)

        @pl.when(steps > 1)
        def _():
            fetch(1)

        if first:
            st_ref[:, :, : RANK + 128] = jnp.zeros((REQ, HEADS, RANK + 128), jnp.float32)
            st_ref[:, :, RANK + 128 :] = jnp.full((REQ, HEADS, 128), -1e30, jnp.float32)
        else:
            st_ref[...] = old_ref[...]
        lax.fori_loop(0, steps, step, 0)

        @pl.when(steps > 1)
        def _():
            drain(steps % 2)

        @pl.when(steps > 0)
        def _():
            drain((steps + 1) % 2)

    smem, vmem, anywhere = (pl.BlockSpec(memory_space=m) for m in (pltpu.SMEM, pltpu.VMEM, pl.ANY))
    state_shape = (REQ, HEADS, RANK + 256)
    in_specs = [smem] * 2 + [anywhere] * total + [vmem] * 2 + [anywhere] * 2
    operands = [counts, codes, *parts, q_lat, q_rope_t]
    aliases = {len(operands): 0, len(operands) + 1: 1}
    operands += list(caches)
    if not first:
        in_specs.append(vmem)
        operands.append(state)
    out_specs = [anywhere, anywhere, vmem]
    out_shape = [jax.ShapeDtypeStruct(c.shape, c.dtype) for c in caches] + [jax.ShapeDtypeStruct(state_shape, jnp.float32)]
    return pl.pallas_call(
        kernel,
        in_specs=in_specs,
        out_specs=out_specs,
        out_shape=out_shape,
        scratch_shapes=[
            pltpu.VMEM((3, ROWS, 128), jnp.bfloat16),
            pltpu.VMEM((2, UNIT, RANK), jnp.bfloat16),
            pltpu.VMEM((2, ROPE, UNIT), jnp.bfloat16),
            pltpu.SemaphoreType.DMA((3,)),
            pltpu.SemaphoreType.DMA((2,)),
            pltpu.SemaphoreType.DMA((2,)),
        ],
        input_output_aliases=aliases,
        cost_estimate=pl.CostEstimate(flops=2 * 10**8, bytes_accessed=8 * 589824, transcendentals=0),
        name="attend",
    )(*operands)


def blank_caches(lens):
    def kernel(len_ref, c_ref, k_ref, c_zero, k_zero, c_sem, k_sem):
        c_zero[...] = jnp.zeros_like(c_zero)
        k_zero[...] = jnp.zeros_like(k_zero)

        def each(act):
            def block(n, _):
                r, s = n // N, n % N

                @pl.when(len_ref[r] < (s + 1) * SEQ)
                def _():
                    at = pl.ds(pl.multiple_of(s * SEQ, SEQ), SEQ)
                    act(pltpu.make_async_copy(c_zero, c_ref.at[r, at, :], c_sem.at[n]))
                    act(pltpu.make_async_copy(k_zero, k_ref.at[r, :, at], k_sem.at[n]))

                return 0

            lax.fori_loop(0, REQ * N, block, 0)

        each(lambda copy: copy.start())
        each(lambda copy: copy.wait())

    return pl.pallas_call(
        kernel,
        in_specs=[pl.BlockSpec(memory_space=pltpu.SMEM)],
        out_specs=[pl.BlockSpec(memory_space=pl.ANY)] * 2,
        out_shape=[
            jax.ShapeDtypeStruct((REQ, N * SEQ, RANK), jnp.bfloat16),
            jax.ShapeDtypeStruct((REQ, ROPE, N * SEQ), jnp.bfloat16),
        ],
        scratch_shapes=[
            pltpu.VMEM((SEQ, RANK), jnp.bfloat16),
            pltpu.VMEM((ROPE, SEQ), jnp.bfloat16),
            pltpu.SemaphoreType.DMA((REQ * N,)),
            pltpu.SemaphoreType.DMA((REQ * N,)),
        ],
        cost_estimate=pl.CostEstimate(flops=4 * 10**8, bytes_accessed=85 * 10**6, transcendentals=0),
        name="blank",
    )(lens)


def count_units(seq_lens):
    valid = jnp.clip(seq_lens[None, :] - SEQ * jnp.arange(N, dtype=jnp.int32)[:, None], 0, SEQ)
    left = valid.reshape(N, CHIPS, 2, REQ)[..., None] - UNIT * jnp.arange(PER, dtype=jnp.int32)
    left = left.transpose(0, 1, 3, 4, 2).reshape(N, CHIPS, SLOTS)
    return left


def split_place(place):
    return place // (2 * PER), place // 2 % PER, place % 2


def pack_tables(me, left, slot):
    have = left > 0
    places = jnp.arange(SLOTS, dtype=jnp.int32)
    chips = me // 2 ^ jnp.arange(CHIPS)
    mine = have[me][chips]
    rank = jnp.sum((mine[:, None, :] & (places[None, :] <= places[:, None])).astype(jnp.int32), axis=-1)
    place = jnp.sum((rank[:, None, :] <= slot[:, :, None]).astype(jnp.int32), axis=-1)
    final = jnp.max(jnp.where(mine, places, 0), axis=-1, keepdims=True)
    req, unit, core = split_place(jnp.minimum(place, final))
    req = (2 * chips[:, None] + core) * REQ + req
    return [req.reshape(-1), unit.reshape(-1), (place < SLOTS).astype(jnp.int32).reshape(-1)]


def attend_tables(me, left, slot, widths, runs):
    places = jnp.arange(SLOTS, dtype=jnp.int32)
    part = jnp.arange(N)
    source = me ^ part
    theirs = left[source, me // 2]
    rank = jnp.sum(((theirs > 0)[:, None, :] & (places[None, :] <= places[:, None])).astype(jnp.int32), axis=-1)
    place = jnp.sum((rank[:, None, :] <= slot[:, :, None]).astype(jnp.int32), axis=-1)
    req, unit, core = split_place(place)
    rows = jnp.sum(jnp.where(place[:, :, None] == places, theirs[:, None, :], 0), axis=-1)
    rows = jnp.where(core == me % 2, jnp.minimum(rows, UNIT), 0)
    starts = np.cumsum([0] + list(widths))[:-1]
    inside = np.concatenate([np.arange(w) for w in widths])
    depth = np.concatenate([np.full(w, i) for run in runs for i, w in enumerate(widths[c] for c in run)])
    code = part[:, None] * 2**22 + rows * 2**9 + req * 2**5 + source[:, None] * PER + unit
    code = jnp.where(rows > 0, code + jnp.asarray((inside * 2**18 + depth * N * 2**22).astype(np.int32)), 0)
    code = jnp.concatenate([code[:, s : s + w].reshape(-1) for w, s in zip(widths, starts)])
    sizes = [N * sum(widths[c] for c in run) for run in runs]
    first = np.cumsum([0] + sizes)[:-1]
    run_of = np.repeat(np.arange(len(runs)), sizes).astype(np.int32)
    same = jnp.asarray(run_of)[:, None] == jnp.asarray(run_of)[None, :]
    number = jnp.arange(len(run_of), dtype=jnp.int32)
    before = jnp.sum((same & (number[None, :] < number[:, None]) & (code > 0)[None, :]).astype(jnp.int32), axis=-1)
    goes_to = jnp.where(code > 0, jnp.asarray(first[run_of].astype(np.int32)) + before, -1)
    codes = jnp.sum(jnp.where(goes_to[None, :] == number[:, None], code[None, :], 0), axis=-1)
    in_run = jnp.asarray(run_of)[None, :] == jnp.arange(len(runs), dtype=jnp.int32)[:, None]
    return codes, jnp.sum((in_run & (code > 0)[None, :]).astype(jnp.int32), axis=-1), first


def pairs(sources, hop):
    return [(s, s ^ hop) for s in sources]


def send(x, pairs):
    return lax.ppermute(x, "x", pairs)


def runs_of(count):
    return [(c,) for c in range(count - 2)] + [(count - 2, count - 1)]


def run_plan(me, left, own_lens, weights, q_lat, q_rope_t):
    plan = PLAN
    widths = [chunk[0] for chunk in plan.chunks]
    count = len(widths)
    runs = runs_of(count)
    pack_tabs = pack_tables(me, left, jnp.asarray(plan.slot)[me])
    part = jnp.arange(N)
    codes, counts, first = attend_tables(me, left, jnp.asarray(plan.slot)[me ^ part, part // 2], widths, runs)
    caches = blank_caches(own_lens)
    landed, owns, twins = [], [], []
    after = []
    for c, (width, kind, along, across, diagonal) in enumerate(plan.chunks):
        staged = norm_pack(width, int(plan.starts[c]), SLOTS, pack_tabs, *weights, after)
        after = [staged[0]]
        sends = list(staged)
        if c >= DEPTH:
            sends, landed[c - DEPTH] = lax.optimization_barrier((sends, landed[c - DEPTH]))
        owns.append(sends[0])
        twins.append(send(sends[0], pairs(ALL, 1)))
        far = send(sends[3], pairs(ALL, 4) if kind == "relay" else pairs(diagonal, 6))
        near = send(sends[1], pairs(UP, 2) + pairs(LOW, 1) if along == UP else pairs(ALL, 2))
        over = send(sends[2], pairs(across, 4))
        landed.append([near, over, far])
    state = None
    for number, run in enumerate(runs):
        parts = []
        for c in run:
            near, over, far = landed[c]
            if plan.chunks[c][1] == "relay":
                far = send(far, pairs(LOW, 2) + pairs(UP, 1))
            parts += [owns[c], twins[c]]
            for x in (near, over, far):
                parts += [x, send(x, pairs(ALL, 1))]
        *caches, state = attend(number, int(first[number]), number == 0, counts, codes, parts, q_lat, q_rope_t, caches, state)
    return caches[0], caches[1], state


def run_extra(step, me, left, weights, q_lat, q_rope_t, caches, state):
    cap = jnp.asarray(PLAN.cap)
    more = step * EXTRA + jnp.arange(EXTRA, dtype=jnp.int32)
    part = jnp.arange(N)
    slot = cap[me][:, None] + more
    staged = norm_pack(EXTRA, 0, EXTRA, pack_tables(me, left, slot), *weights, [])
    slot = cap[me ^ part, part // 2][:, None] + more
    codes, counts, _ = attend_tables(me, left, slot, [EXTRA], [(0,)])
    parts = []
    for q, x in enumerate(staged):
        x = lax.ppermute(x, "x", pairs(ALL, 2 * q)) if q else x
        parts += [x, lax.ppermute(x, "x", pairs(ALL, 1))]
    return attend(0, 0, False, counts, codes, parts, q_lat, q_rope_t, caches, state)


def local_step(c_raw, k_raw, norm_gain, rope_cos, rope_sin, seq_lens, q_lat, q_rope):
    me = lax.axis_index("x")
    left = count_units(seq_lens)
    own_lens = lax.dynamic_slice_in_dim(seq_lens, me * REQ, REQ)
    weights = (c_raw, jnp.swapaxes(k_raw, 1, 2), norm_gain[None, :], rope_cos.T, rope_sin.T)
    q_rope_t = jnp.swapaxes(q_rope, 1, 2)
    c_cache, k_cache_t, state = run_plan(me, left, own_lens, weights, q_lat, q_rope_t)
    need = jnp.sum((left > 0).astype(jnp.int32), axis=-1)
    cap = np.stack([[PLAN.cap[s, (s // 2) ^ chip] for chip in range(CHIPS)] for s in range(N)])
    steps = (jnp.maximum(jnp.max(need - jnp.asarray(cap)), 0) + EXTRA - 1) // EXTRA

    def body(carry):
        step, *caches, state = carry
        return step + 1, *run_extra(step, me, left, weights, q_lat, q_rope_t, caches, state)

    _, c_cache, k_cache_t, state = lax.while_loop(lambda carry: carry[0] < steps, body, (jnp.int32(0), c_cache, k_cache_t, state))
    o_lat = (state[:, :, :RANK] / state[:, :, RANK : RANK + 1]).astype(jnp.bfloat16)
    return c_cache, jnp.swapaxes(k_cache_t, 1, 2), o_lat


def solution(mesh):
    seq_spec = P("dp", "x", None)
    req_spec = P(("dp", "x"), None, None)
    return jax.shard_map(
        local_step,
        mesh=mesh,
        in_specs=(seq_spec, seq_spec, P(None), P("x", None), P("x", None), P("dp"), req_spec, req_spec),
        out_specs=(req_spec, req_spec, req_spec),
        check_vma=False,
    )
```

```python
import jax
import jax.numpy as jnp
import numpy as np
from jax import lax
from jax.experimental import pallas as pl
from jax.experimental.pallas import tpu as pltpu
from jax.sharding import PartitionSpec as P

NORM_EPS = 1e-6
N = 8
CHIPS = 4
REQ = 12
SEQ = 768
RANK = 512
ROPE = 64
HEADS = 128
UNIT = 256
PER = SEQ // UNIT
PIECES = RANK // 128
HALVES = UNIT // 128
ROWS = PIECES * UNIT + HALVES * ROPE
SLOTS = 2 * REQ * PER
NONE = 10**6
ATTN_SCALE = (RANK + ROPE) ** -0.5
DEPTH = 2


SPILL = 8
SPILLERS = (2, 3)


class Plan:
    def __init__(self, chunks):
        self.chunks = chunks
        self.starts = np.cumsum([0] + [c[0] for c in chunks])[:-1]
        assert sum(c[0] for c in chunks) == SLOTS
        self.slot = np.full((N, CHIPS, SLOTS), NONE, np.int32)
        self.cap = np.zeros((N, CHIPS), np.int32)
        for s in range(N):
            for q in range(CHIPS):
                spills = s in SPILLERS and q in (2, 3)
                for c in sorted(range(len(chunks)), key=lambda c: spills and c == SPILL):
                    chunk, start, width = chunks[c], self.starts[c], chunks[c][0]
                    if q == 0 or s in chunk[q + 1]:
                        self.slot[s, q, start : start + width] = self.cap[s, q] + np.arange(width)
                        self.cap[s, q] += width


ALL = (0, 1, 2, 3, 4, 5, 6, 7)
UP = (0, 1, 2, 3)
LOW = (4, 5, 6, 7)


NO_CHIP1 = (0, 1, 4, 5, 6, 7)
NO_3 = (0, 1, 2, 4, 5, 6, 7)


def direct(width):
    return width, "direct", ALL, ALL, ALL


def relay(width):
    return width, "relay", UP, ALL, UP


def no_chip1(width):
    return width, "direct", ALL, NO_CHIP1, NO_CHIP1


def no_3(width):
    return width, "direct", ALL, NO_3, NO_3


def end(width):
    return width, "direct", UP, ALL, UP


PLAN = Plan(
    [direct(2), direct(4), direct(6), relay(7), no_chip1(5), relay(6), no_chip1(4), no_3(9)]
    + [direct(8), direct(8), direct(7), end(4), end(2)]
)
ROOM = PLAN.chunks[SPILL][0]
EXTRA = 4


def norm_pack(width, start, stride, tabs, c_raw, k_t, gain, cos_t, sin_t, after):
    steps = CHIPS * width

    def kernel(req_ref, unit_ref, ok_ref, c_ref, k_ref, g_ref, cos_ref, sin_ref, *refs):
        outs, (buf, sem) = refs[len(after) : len(after) + CHIPS], refs[-2:]
        n = pl.program_id(0)
        q, j = n // width, n % width
        ok_at = lambda m: ok_ref[m // width * stride + start + m % width] > 0
        drain = lambda m: pltpu.make_async_copy(buf.at[m % 2], outs[0].at[0], sem.at[m % 2]).wait()
        slot = n % 2

        @pl.when((n >= 2) & ok_at(jnp.maximum(n - 2, 0)))
        def _():
            drain(n)

        @pl.when(ok_at(n))
        def _():
            key = k_ref[0].astype(jnp.float32)
            lo, hi = key[: ROPE // 2], key[ROPE // 2 :]
            cos, sin = cos_ref[...], sin_ref[...]
            rot = jnp.concatenate([lo * cos - hi * sin, hi * cos + lo * sin], axis=0).astype(jnp.bfloat16)
            for p in range(HALVES):
                at = PIECES * UNIT + p * ROPE
                buf[slot, at : at + ROPE, :] = rot[:, p * 128 : (p + 1) * 128]
                x = c_ref[0, p * 128 : (p + 1) * 128, :].astype(jnp.float32)
                inv = lax.rsqrt(jnp.mean(x * x, axis=-1, keepdims=True) + NORM_EPS)
                y = (x * inv * g_ref[...].astype(jnp.float32)).astype(jnp.bfloat16)
                for i in range(PIECES):
                    at = i * UNIT + p * 128
                    buf[slot, at : at + 128, :] = y[:, i * 128 : (i + 1) * 128]
            for mine in range(CHIPS):

                @pl.when(q == mine)
                def _(mine=mine):
                    pltpu.make_async_copy(buf.at[slot], outs[mine].at[j], sem.at[slot]).start()

        @pl.when(n == steps - 1)
        def _():
            @pl.when(ok_at(n - 1))
            def _():
                drain(n - 1)

            @pl.when(ok_at(n))
            def _():
                drain(n)

    def at(n):
        return n // width * stride + start + n % width

    grid_spec = pltpu.PrefetchScalarGridSpec(
        num_scalar_prefetch=3,
        grid=(steps,),
        in_specs=[
            pl.BlockSpec((1, UNIT, RANK), lambda n, req, unit, ok: (req[at(n)], unit[at(n)], 0)),
            pl.BlockSpec((1, ROPE, UNIT), lambda n, req, unit, ok: (req[at(n)], 0, unit[at(n)])),
            pl.BlockSpec((1, RANK), lambda n, *_: (0, 0)),
            pl.BlockSpec((ROPE // 2, UNIT), lambda n, req, unit, ok: (0, unit[at(n)])),
            pl.BlockSpec((ROPE // 2, UNIT), lambda n, req, unit, ok: (0, unit[at(n)])),
        ]
        + [pl.BlockSpec(memory_space=pl.ANY)] * len(after),
        out_specs=[pl.BlockSpec(memory_space=pl.ANY)] * CHIPS,
        scratch_shapes=[pltpu.VMEM((2, ROWS, 128), jnp.bfloat16), pltpu.SemaphoreType.DMA((2,))],
    )
    return pl.pallas_call(
        kernel,
        grid_spec=grid_spec,
        out_shape=[jax.ShapeDtypeStruct((width, ROWS, 128), jnp.bfloat16)] * CHIPS,
        cost_estimate=pl.CostEstimate(flops=width * 10**8, bytes_accessed=width * 4 * 589824, transcendentals=0),
        name="norm_pack",
    )(*tabs, c_raw, k_t, gain, cos_t, sin_t, *after)


def attend(chunk, start, first, last, counts, codes, parts, q_lat, q_rope_t, caches, state):
    total = len(parts)

    def kernel(count_ref, code_ref, *refs):
        part_refs, (qa_ref, qr_ref) = refs[:total], refs[total : total + 2]
        old_ref = None if first else refs[total + 4]
        outs = refs[total + (4 if first else 5) :]
        c_out, k_out, st_ref = outs[:3]
        buf, c_buf, k_buf, in_sem, c_sem, k_sem = outs[-6:]
        steps = count_ref[chunk]

        def fetch(n):
            code = code_ref[start + n]
            part, place = code // 2**22, code // 2**18 % 16
            for k in range(total):

                @pl.when(part == k)
                def _(k=k):
                    pltpu.make_async_copy(part_refs[k].at[place], buf.at[n % 3], in_sem.at[n % 3]).start()

        def drain(slot):
            pltpu.make_async_copy(c_buf.at[slot], c_out.at[0, pl.ds(0, UNIT), :], c_sem.at[slot]).wait()
            pltpu.make_async_copy(k_buf.at[slot], k_out.at[0, :, pl.ds(0, UNIT)], k_sem.at[slot]).wait()

        def step(n, _):
            code = code_ref[start + n]
            left, r = code // 2**9 % 2**9, code // 2**5 % 16
            at = pl.ds(pl.multiple_of(code % 2**5 * UNIT, UNIT), UNIT)
            slot = n % 2

            @pl.when(n + 2 < steps)
            def _():
                fetch(n + 2)

            pltpu.make_async_copy(part_refs[0].at[0], buf.at[n % 3], in_sem.at[n % 3]).wait()

            @pl.when(n >= 2)
            def _():
                drain(slot)

            row_ok = lax.broadcasted_iota(jnp.int32, (UNIT, 1), 0) < left
            lane_ok = lax.broadcasted_iota(jnp.int32, (1, UNIT), 1) < left
            for i in range(PIECES):
                piece = jnp.where(row_ok, buf[n % 3, i * UNIT : (i + 1) * UNIT, :].astype(jnp.float32), 0.0)
                c_buf[slot, :, i * 128 : (i + 1) * 128] = piece.astype(jnp.bfloat16)
            for p in range(HALVES):
                base = PIECES * UNIT + p * ROPE
                key = buf[n % 3, base : base + ROPE, :].astype(jnp.float32)
                key = jnp.where(lane_ok[:, p * 128 : (p + 1) * 128], key, 0.0)
                k_buf[slot, :, p * 128 : (p + 1) * 128] = key.astype(jnp.bfloat16)
            pltpu.make_async_copy(c_buf.at[slot], c_out.at[r, at, :], c_sem.at[slot]).start()
            pltpu.make_async_copy(k_buf.at[slot], k_out.at[r, :, at], k_sem.at[slot]).start()

            c = c_buf[slot]
            scores = lax.dot_general(qa_ref[r], c, (((1,), (1,)), ((), ())), preferred_element_type=jnp.float32)
            scores += lax.dot_general(qr_ref[r], k_buf[slot], (((0,), (0,)), ((), ())), preferred_element_type=jnp.float32)
            scores = jnp.where(lane_ok, scores * ATTN_SCALE, -1e30)
            l_old = st_ref[r, :, RANK : RANK + 1]
            m_old = st_ref[r, :, RANK + 128 : RANK + 129]
            m_new = jnp.maximum(m_old, jnp.max(scores, axis=-1, keepdims=True))
            weights = jnp.exp(scores - m_new)
            decay = jnp.exp(m_old - m_new)
            l_new = l_old * decay + jnp.sum(weights, axis=-1, keepdims=True)
            st_ref[r, :, RANK : RANK + 128] = jnp.broadcast_to(l_new, (HEADS, 128))
            st_ref[r, :, RANK + 128 :] = jnp.broadcast_to(m_new, (HEADS, 128))
            st_ref[r, :, :RANK] = st_ref[r, :, :RANK] * decay + jnp.dot(
                weights.astype(jnp.bfloat16), c, preferred_element_type=jnp.float32
            )
            return 0

        @pl.when(steps > 0)
        def _():
            fetch(0)

        @pl.when(steps > 1)
        def _():
            fetch(1)

        if first:
            st_ref[:, :, : RANK + 128] = jnp.zeros((REQ, HEADS, RANK + 128), jnp.float32)
            st_ref[:, :, RANK + 128 :] = jnp.full((REQ, HEADS, 128), -1e30, jnp.float32)
        else:
            st_ref[...] = old_ref[...]
        lax.fori_loop(0, steps, step, 0)

        @pl.when(steps > 1)
        def _():
            drain(steps % 2)

        @pl.when(steps > 0)
        def _():
            drain((steps + 1) % 2)

        if last:
            o_ref = outs[3]

            def finish(r, _):
                o_ref[r] = (st_ref[r, :, :RANK] / st_ref[r, :, RANK : RANK + 1]).astype(jnp.bfloat16)
                return 0

            lax.fori_loop(0, REQ, finish, 0)

    smem, vmem, anywhere = (pl.BlockSpec(memory_space=m) for m in (pltpu.SMEM, pltpu.VMEM, pl.ANY))
    state_shape = (REQ, HEADS, RANK + 256)
    in_specs = [smem] * 2 + [anywhere] * total + [vmem] * 2 + [anywhere] * 2
    operands = [counts, codes, *parts, q_lat, q_rope_t]
    aliases = {len(operands): 0, len(operands) + 1: 1}
    operands += list(caches)
    if not first:
        in_specs.append(vmem)
        operands.append(state)
    out_specs = [anywhere, anywhere, vmem]
    out_shape = [jax.ShapeDtypeStruct(c.shape, c.dtype) for c in caches] + [jax.ShapeDtypeStruct(state_shape, jnp.float32)]
    if last:
        out_specs.append(vmem)
        out_shape.append(jax.ShapeDtypeStruct((REQ, HEADS, RANK), jnp.bfloat16))
    return pl.pallas_call(
        kernel,
        in_specs=in_specs,
        out_specs=out_specs,
        out_shape=out_shape,
        scratch_shapes=[
            pltpu.VMEM((3, ROWS, 128), jnp.bfloat16),
            pltpu.VMEM((2, UNIT, RANK), jnp.bfloat16),
            pltpu.VMEM((2, ROPE, UNIT), jnp.bfloat16),
            pltpu.SemaphoreType.DMA((3,)),
            pltpu.SemaphoreType.DMA((2,)),
            pltpu.SemaphoreType.DMA((2,)),
        ],
        input_output_aliases=aliases,
        cost_estimate=pl.CostEstimate(flops=2 * 10**8, bytes_accessed=8 * 589824, transcendentals=0),
        name="attend",
    )(*operands)


def blank_caches(lens):
    def kernel(len_ref, c_ref, k_ref, c_zero, k_zero, c_sem, k_sem):
        c_zero[...] = jnp.zeros_like(c_zero)
        k_zero[...] = jnp.zeros_like(k_zero)

        def each(act):
            def block(n, _):
                r, s = n // N, n % N

                @pl.when(len_ref[r] < (s + 1) * SEQ)
                def _():
                    at = pl.ds(pl.multiple_of(s * SEQ, SEQ), SEQ)
                    act(pltpu.make_async_copy(c_zero, c_ref.at[r, at, :], c_sem.at[n]))
                    act(pltpu.make_async_copy(k_zero, k_ref.at[r, :, at], k_sem.at[n]))

                return 0

            lax.fori_loop(0, REQ * N, block, 0)

        each(lambda copy: copy.start())
        each(lambda copy: copy.wait())

    return pl.pallas_call(
        kernel,
        in_specs=[pl.BlockSpec(memory_space=pltpu.SMEM)],
        out_specs=[pl.BlockSpec(memory_space=pl.ANY)] * 2,
        out_shape=[
            jax.ShapeDtypeStruct((REQ, N * SEQ, RANK), jnp.bfloat16),
            jax.ShapeDtypeStruct((REQ, ROPE, N * SEQ), jnp.bfloat16),
        ],
        scratch_shapes=[
            pltpu.VMEM((SEQ, RANK), jnp.bfloat16),
            pltpu.VMEM((ROPE, SEQ), jnp.bfloat16),
            pltpu.SemaphoreType.DMA((REQ * N,)),
            pltpu.SemaphoreType.DMA((REQ * N,)),
        ],
        cost_estimate=pl.CostEstimate(flops=4 * 10**8, bytes_accessed=85 * 10**6, transcendentals=0),
        name="blank",
    )(lens)


def count_units(seq_lens):
    valid = jnp.clip(seq_lens[None, :] - SEQ * jnp.arange(N, dtype=jnp.int32)[:, None], 0, SEQ)
    left = valid.reshape(N, CHIPS, 2, REQ)[..., None] - UNIT * jnp.arange(PER, dtype=jnp.int32)
    left = left.transpose(0, 1, 3, 4, 2).reshape(N, CHIPS, SLOTS)
    return left


def split_place(place):
    return place // (2 * PER), place // 2 % PER, place % 2


def rank_of(have):
    places = jnp.arange(SLOTS, dtype=jnp.int32)
    return jnp.sum((have[:, None, :] & (places[None, :] <= places[:, None])).astype(jnp.int32), axis=-1)


def place_of(rank, slot):
    return jnp.sum((rank[:, None, :] <= slot[:, :, None]).astype(jnp.int32), axis=-1)


def pack_tables(me, left, slot, spill):
    have = left > 0
    places = jnp.arange(SLOTS, dtype=jnp.int32)
    chips = me // 2 ^ jnp.arange(CHIPS)
    mine = have[me][chips]
    rank = rank_of(mine)
    place = place_of(rank, slot)
    to = jnp.broadcast_to(chips[:, None], place.shape)
    if spill is not None:
        other = np.array([0, 1, 3, 2])
        spilt = spill & (place == SLOTS)
        cap = jnp.asarray(PLAN.cap)[me][:, None]
        place = jnp.where(spilt, place_of(rank[other], 2 * cap - 1 - slot), place)
        to = jnp.where(spilt, chips[other][:, None], to)
    final = jnp.max(jnp.where(mine, places, 0), axis=-1, keepdims=True)
    ok = place < SLOTS
    to = jnp.where(ok, to, chips[:, None])
    req, unit, core = split_place(jnp.where(ok, place, final))
    req = (2 * to + core) * REQ + req
    return [req.reshape(-1), unit.reshape(-1), ok.astype(jnp.int32).reshape(-1)]


def unit_codes(me, source, theirs, slot, valid):
    places = jnp.arange(SLOTS, dtype=jnp.int32)
    place = place_of(rank_of(theirs > 0), slot)
    req, unit, core = split_place(place)
    rows = jnp.sum(jnp.where(place[:, :, None] == places, theirs[:, None, :], 0), axis=-1)
    rows = jnp.where(valid & (core == me % 2), jnp.minimum(rows, UNIT), 0)
    return jnp.where(rows > 0, rows * 2**9 + req * 2**5 + source[:, None] * PER + unit, 0)


def attend_tables(me, left, slot, widths, runs, spill):
    part = jnp.arange(N)
    source = me ^ part
    chip = me // 2
    code = unit_codes(me, source, left[source, chip], slot, True)
    starts = np.cumsum([0] + list(widths))[:-1]
    inside = np.concatenate([np.arange(w) for w in widths])
    depth = np.concatenate([np.full(w, i) for run in runs for i, w in enumerate(widths[c] for c in run)])
    extra = jnp.asarray((inside * 2**18 + depth * N * 2**22).astype(np.int32))
    code = jnp.where(code > 0, code + part[:, None] * 2**22 + extra, 0)
    pieces = [code[:, s : s + w].reshape(-1) for w, s in zip(widths, starts)]
    sizes = [N * sum(widths[c] for c in run) for run in runs]
    if spill:
        source = jnp.where(chip == 3, me ^ 4, me ^ 6) ^ jnp.arange(2)
        cap = jnp.asarray(PLAN.cap[:, 2])[source][:, None]
        unused = jnp.arange(ROOM, dtype=jnp.int32)
        spilt = cap - ROOM + unused
        their_need = jnp.sum((left[source, chip ^ 1] > 0).astype(jnp.int32), axis=-1, keepdims=True)
        valid = (chip >= 2) & (spilt >= their_need)
        more = unit_codes(me, source, left[source, chip], 2 * cap - 1 - spilt, valid)
        more = jnp.where(more > 0, more + (N + jnp.arange(2))[:, None] * 2**22 + unused * 2**18, 0)
        pieces.insert(SPILL + 1, more.reshape(-1))
        sizes[SPILL] += 2 * ROOM
    code = jnp.concatenate(pieces)
    first = np.cumsum([0] + sizes)[:-1]
    run_of = np.repeat(np.arange(len(runs)), sizes).astype(np.int32)
    same = jnp.asarray(run_of)[:, None] == jnp.asarray(run_of)[None, :]
    number = jnp.arange(len(run_of), dtype=jnp.int32)
    before = jnp.sum((same & (number[None, :] < number[:, None]) & (code > 0)[None, :]).astype(jnp.int32), axis=-1)
    goes_to = jnp.where(code > 0, jnp.asarray(first[run_of].astype(np.int32)) + before, -1)
    codes = jnp.sum(jnp.where(goes_to[None, :] == number[:, None], code[None, :], 0), axis=-1)
    in_run = jnp.asarray(run_of)[None, :] == jnp.arange(len(runs), dtype=jnp.int32)[:, None]
    return codes, jnp.sum((in_run & (code > 0)[None, :]).astype(jnp.int32), axis=-1), first


def pairs(sources, hop):
    return [(s, s ^ hop) for s in sources]


def send(x, pairs):
    return lax.ppermute(x, "x", pairs)


def runs_of(count):
    return [(c,) for c in range(count - 2)] + [(count - 2, count - 1)]


def run_plan(me, left, own_lens, weights, q_lat, q_rope_t):
    plan = PLAN
    widths = [chunk[0] for chunk in plan.chunks]
    count = len(widths)
    runs = runs_of(count)
    spill = np.zeros((N, CHIPS, SLOTS), bool)
    spill[np.ix_(SPILLERS, (2, 3), range(plan.starts[SPILL], plan.starts[SPILL] + ROOM))] = True
    pack_tabs = pack_tables(me, left, jnp.asarray(plan.slot)[me], jnp.asarray(spill)[me])
    part = jnp.arange(N)
    codes, counts, first = attend_tables(me, left, jnp.asarray(plan.slot)[me ^ part, part // 2], widths, runs, True)
    caches = blank_caches(own_lens)
    landed, owns, twins = [], [], []
    after = []
    for c, (width, kind, along, across, diagonal) in enumerate(plan.chunks):
        staged = norm_pack(width, int(plan.starts[c]), SLOTS, pack_tabs, *weights, after)
        after = [staged[0]]
        sends = list(staged)
        if c >= DEPTH:
            sends, landed[c - DEPTH] = lax.optimization_barrier((sends, landed[c - DEPTH]))
        owns.append(sends[0])
        twins.append(send(sends[0], pairs(ALL, 1)))
        far = send(sends[3], pairs(ALL, 4) if kind == "relay" else pairs(diagonal, 6))
        near = send(sends[1], pairs(UP, 2) + pairs(LOW, 1) if along == UP else pairs(ALL, 2))
        over = send(sends[2], pairs(across, 4))
        landed.append([near, over, far])
    state = None
    for number, run in enumerate(runs):
        parts = []
        for c in run:
            near, over, far = landed[c]
            if plan.chunks[c][1] == "relay":
                far = send(far, pairs(LOW, 2) + pairs(UP, 1))
                far, landed[c + 1] = lax.optimization_barrier((far, landed[c + 1]))
            parts += [owns[c], twins[c]]
            for x in (near, over, far):
                parts += [x, send(x, pairs(ALL, 1))]
            if c == SPILL:
                x = send(jnp.where(me // 2 == 3, over, far), pairs(LOW, 2) + pairs(UP, 1))
                x, landed[c + 1] = lax.optimization_barrier((x, landed[c + 1]))
                parts += [x, send(x, pairs(ALL, 1))]
        got = attend(number, int(first[number]), number == 0, number == len(runs) - 1, counts, codes, parts, q_lat, q_rope_t, caches, state)
        caches, state = got[:2], got[2]
    return got


def run_extra(step, cap, me, left, weights, q_lat, q_rope_t, caches, state):
    more = step * EXTRA + jnp.arange(EXTRA, dtype=jnp.int32)
    part = jnp.arange(N)
    slot = cap[me][:, None] + more
    staged = norm_pack(EXTRA, 0, EXTRA, pack_tables(me, left, slot, None), *weights, [])
    slot = cap[me ^ part, part // 2][:, None] + more
    codes, counts, _ = attend_tables(me, left, slot, [EXTRA], [(0,)], False)
    parts = []
    for q, x in enumerate(staged):
        x = lax.ppermute(x, "x", pairs(ALL, 2 * q)) if q else x
        parts += [x, lax.ppermute(x, "x", pairs(ALL, 1))]
    return attend(0, 0, False, True, counts, codes, parts, q_lat, q_rope_t, caches, state)


def local_step(c_raw, k_raw, norm_gain, rope_cos, rope_sin, seq_lens, q_lat, q_rope):
    me = lax.axis_index("x")
    left = count_units(seq_lens)
    own_lens = lax.dynamic_slice_in_dim(seq_lens, me * REQ, REQ)
    weights = (c_raw, jnp.swapaxes(k_raw, 1, 2), norm_gain[None, :], rope_cos.T, rope_sin.T)
    q_rope_t = jnp.swapaxes(q_rope, 1, 2)
    done = run_plan(me, left, own_lens, weights, q_lat, q_rope_t)
    need = jnp.sum((left > 0).astype(jnp.int32), axis=-1)
    to = np.arange(N)[:, None] // 2 ^ np.arange(CHIPS)
    need = jnp.sum(need[:, None, :] * jnp.asarray(to[:, :, None] == np.arange(CHIPS)), axis=-1)
    spills = np.isin(np.arange(N), SPILLERS)[:, None] & np.isin(np.arange(CHIPS), (2, 3))
    room = jnp.clip(jnp.asarray(PLAN.cap) - need[:, np.array([0, 1, 3, 2])], 0, ROOM)
    cap = jnp.asarray(PLAN.cap) + jnp.where(jnp.asarray(spills), room, 0)
    steps = (jnp.maximum(jnp.max(need - cap), 0) + EXTRA - 1) // EXTRA

    def body(carry):
        step, c_cache, k_cache_t, state, _ = carry
        return step + 1, *run_extra(step, cap, me, left, weights, q_lat, q_rope_t, (c_cache, k_cache_t), state)

    _, c_cache, k_cache_t, _, o_lat = lax.while_loop(lambda carry: carry[0] < steps, body, (jnp.int32(0), *done))
    return c_cache, jnp.swapaxes(k_cache_t, 1, 2), o_lat


def solution(mesh):
    seq_spec = P("dp", "x", None)
    req_spec = P(("dp", "x"), None, None)
    return jax.shard_map(
        local_step,
        mesh=mesh,
        in_specs=(seq_spec, seq_spec, P(None), P("x", None), P("x", None), P("dp"), req_spec, req_spec),
        out_specs=(req_spec, req_spec, req_spec),
        check_vma=False,
    )
```

```python
import jax
import jax.numpy as jnp
import numpy as np
from jax import lax
from jax.experimental import pallas as pl
from jax.experimental.pallas import tpu as pltpu
from jax.sharding import PartitionSpec as P

NORM_EPS = 1e-6
N = 8
CHIPS = 4
REQ = 12
SEQ = 768
RANK = 512
ROPE = 64
HEADS = 128
UNIT = 256
PER = SEQ // UNIT
PIECES = RANK // 128
HALVES = UNIT // 128
ROWS = PIECES * UNIT + HALVES * ROPE
SLOTS = 2 * REQ * PER
NONE = 10**6
ATTN_SCALE = (RANK + ROPE) ** -0.5
DEPTH = 2


SPILL = 8
SPILLERS = (2, 3)


class Plan:
    def __init__(self, chunks):
        self.chunks = chunks
        self.starts = np.cumsum([0] + [c[0] for c in chunks])[:-1]
        assert sum(c[0] for c in chunks) == SLOTS
        self.slot = np.full((N, CHIPS, SLOTS), NONE, np.int32)
        self.cap = np.zeros((N, CHIPS), np.int32)
        for s in range(N):
            for q in range(CHIPS):
                spills = s in SPILLERS and q in (2, 3)
                for c in sorted(range(len(chunks)), key=lambda c: spills and c == SPILL):
                    chunk, start, width = chunks[c], self.starts[c], chunks[c][0]
                    if q == 0 or s in chunk[q + 1]:
                        self.slot[s, q, start : start + width] = self.cap[s, q] + np.arange(width)
                        self.cap[s, q] += width


ALL = (0, 1, 2, 3, 4, 5, 6, 7)
UP = (0, 1, 2, 3)
LOW = (4, 5, 6, 7)


NO_CHIP1 = (0, 1, 4, 5, 6, 7)
NO_3 = (0, 1, 2, 4, 5, 6, 7)


def direct(width):
    return width, "direct", ALL, ALL, ALL


def relay(width):
    return width, "relay", UP, ALL, UP


def no_chip1(width):
    return width, "direct", ALL, NO_CHIP1, NO_CHIP1


def no_3(width):
    return width, "direct", ALL, NO_3, NO_3


def light(width, among):
    return width, "direct", among, ALL, among


def end(width):
    return width, "direct", UP, ALL, UP


PLAN = Plan(
    [direct(2), direct(4), direct(6), relay(7), no_chip1(5), relay(6), no_chip1(4), no_3(9)]
    + [direct(8), light(8, ALL[:5]), light(7, ALL[:6]), end(4), end(2)]
)
ROOM = PLAN.chunks[SPILL][0]
EXTRA = 4


def norm_pack(width, start, stride, tabs, c_raw, k_t, gain, cos_t, sin_t, after):
    steps = CHIPS * width

    def kernel(req_ref, unit_ref, ok_ref, c_ref, k_ref, g_ref, cos_ref, sin_ref, *refs):
        outs, (buf, sem) = refs[len(after) : len(after) + CHIPS], refs[-2:]
        n = pl.program_id(0)
        q, j = n // width, n % width
        ok_at = lambda m: ok_ref[m // width * stride + start + m % width] > 0
        drain = lambda m: pltpu.make_async_copy(buf.at[m % 2], outs[0].at[0], sem.at[m % 2]).wait()
        slot = n % 2

        @pl.when((n >= 2) & ok_at(jnp.maximum(n - 2, 0)))
        def _():
            drain(n)

        @pl.when(ok_at(n))
        def _():
            key = k_ref[0].astype(jnp.float32)
            lo, hi = key[: ROPE // 2], key[ROPE // 2 :]
            cos, sin = cos_ref[...], sin_ref[...]
            rot = jnp.concatenate([lo * cos - hi * sin, hi * cos + lo * sin], axis=0).astype(jnp.bfloat16)
            for p in range(HALVES):
                at = PIECES * UNIT + p * ROPE
                buf[slot, at : at + ROPE, :] = rot[:, p * 128 : (p + 1) * 128]
                x = c_ref[0, p * 128 : (p + 1) * 128, :].astype(jnp.float32)
                inv = lax.rsqrt(jnp.mean(x * x, axis=-1, keepdims=True) + NORM_EPS)
                y = (x * inv * g_ref[...].astype(jnp.float32)).astype(jnp.bfloat16)
                for i in range(PIECES):
                    at = i * UNIT + p * 128
                    buf[slot, at : at + 128, :] = y[:, i * 128 : (i + 1) * 128]
            for mine in range(CHIPS):

                @pl.when(q == mine)
                def _(mine=mine):
                    pltpu.make_async_copy(buf.at[slot], outs[mine].at[j], sem.at[slot]).start()

        @pl.when(n == steps - 1)
        def _():
            @pl.when(ok_at(n - 1))
            def _():
                drain(n - 1)

            @pl.when(ok_at(n))
            def _():
                drain(n)

    def at(n):
        return n // width * stride + start + n % width

    grid_spec = pltpu.PrefetchScalarGridSpec(
        num_scalar_prefetch=3,
        grid=(steps,),
        in_specs=[
            pl.BlockSpec((1, UNIT, RANK), lambda n, req, unit, ok: (req[at(n)], unit[at(n)], 0)),
            pl.BlockSpec((1, ROPE, UNIT), lambda n, req, unit, ok: (req[at(n)], 0, unit[at(n)])),
            pl.BlockSpec((1, RANK), lambda n, *_: (0, 0)),
            pl.BlockSpec((ROPE // 2, UNIT), lambda n, req, unit, ok: (0, unit[at(n)])),
            pl.BlockSpec((ROPE // 2, UNIT), lambda n, req, unit, ok: (0, unit[at(n)])),
        ]
        + [pl.BlockSpec(memory_space=pl.ANY)] * len(after),
        out_specs=[pl.BlockSpec(memory_space=pl.ANY)] * CHIPS,
        scratch_shapes=[pltpu.VMEM((2, ROWS, 128), jnp.bfloat16), pltpu.SemaphoreType.DMA((2,))],
    )
    return pl.pallas_call(
        kernel,
        grid_spec=grid_spec,
        out_shape=[jax.ShapeDtypeStruct((width, ROWS, 128), jnp.bfloat16)] * CHIPS,
        cost_estimate=pl.CostEstimate(flops=width * 10**8, bytes_accessed=width * 4 * 589824, transcendentals=0),
        name="norm_pack",
    )(*tabs, c_raw, k_t, gain, cos_t, sin_t, *after)


def attend(chunk, start, first, last, counts, codes, parts, q_lat, q_rope_t, caches, state):
    total = len(parts)

    def kernel(count_ref, code_ref, *refs):
        part_refs, (qa_ref, qr_ref) = refs[:total], refs[total : total + 2]
        old_ref = None if first else refs[total + 4]
        outs = refs[total + (4 if first else 5) :]
        c_out, k_out, st_ref = outs[:3]
        buf, c_buf, k_buf, in_sem, c_sem, k_sem = outs[-6:]
        steps = count_ref[chunk]

        def fetch(n):
            code = code_ref[start + n]
            part, place = code // 2**22, code // 2**18 % 16
            for k in range(total):

                @pl.when(part == k)
                def _(k=k):
                    pltpu.make_async_copy(part_refs[k].at[place], buf.at[n % 3], in_sem.at[n % 3]).start()

        def drain(slot):
            pltpu.make_async_copy(c_buf.at[slot], c_out.at[0, pl.ds(0, UNIT), :], c_sem.at[slot]).wait()
            pltpu.make_async_copy(k_buf.at[slot], k_out.at[0, :, pl.ds(0, UNIT)], k_sem.at[slot]).wait()

        def step(n, _):
            code = code_ref[start + n]
            left, r = code // 2**9 % 2**9, code // 2**5 % 16
            at = pl.ds(pl.multiple_of(code % 2**5 * UNIT, UNIT), UNIT)
            slot = n % 2

            @pl.when(n + 2 < steps)
            def _():
                fetch(n + 2)

            pltpu.make_async_copy(part_refs[0].at[0], buf.at[n % 3], in_sem.at[n % 3]).wait()

            @pl.when(n >= 2)
            def _():
                drain(slot)

            row_ok = lax.broadcasted_iota(jnp.int32, (UNIT, 1), 0) < left
            lane_ok = lax.broadcasted_iota(jnp.int32, (1, UNIT), 1) < left
            for i in range(PIECES):
                piece = jnp.where(row_ok, buf[n % 3, i * UNIT : (i + 1) * UNIT, :].astype(jnp.float32), 0.0)
                c_buf[slot, :, i * 128 : (i + 1) * 128] = piece.astype(jnp.bfloat16)
            for p in range(HALVES):
                base = PIECES * UNIT + p * ROPE
                key = buf[n % 3, base : base + ROPE, :].astype(jnp.float32)
                key = jnp.where(lane_ok[:, p * 128 : (p + 1) * 128], key, 0.0)
                k_buf[slot, :, p * 128 : (p + 1) * 128] = key.astype(jnp.bfloat16)
            pltpu.make_async_copy(c_buf.at[slot], c_out.at[r, at, :], c_sem.at[slot]).start()
            pltpu.make_async_copy(k_buf.at[slot], k_out.at[r, :, at], k_sem.at[slot]).start()

            c = c_buf[slot]
            scores = lax.dot_general(qa_ref[r], c, (((1,), (1,)), ((), ())), preferred_element_type=jnp.float32)
            scores += lax.dot_general(qr_ref[r], k_buf[slot], (((0,), (0,)), ((), ())), preferred_element_type=jnp.float32)
            scores = jnp.where(lane_ok, scores * ATTN_SCALE, -1e30)
            l_old = st_ref[r, :, RANK : RANK + 1]
            m_old = st_ref[r, :, RANK + 128 : RANK + 129]
            m_new = jnp.maximum(m_old, jnp.max(scores, axis=-1, keepdims=True))
            weights = jnp.exp(scores - m_new)
            decay = jnp.exp(m_old - m_new)
            l_new = l_old * decay + jnp.sum(weights, axis=-1, keepdims=True)
            st_ref[r, :, RANK : RANK + 128] = jnp.broadcast_to(l_new, (HEADS, 128))
            st_ref[r, :, RANK + 128 :] = jnp.broadcast_to(m_new, (HEADS, 128))
            st_ref[r, :, :RANK] = st_ref[r, :, :RANK] * decay + jnp.dot(
                weights.astype(jnp.bfloat16), c, preferred_element_type=jnp.float32
            )
            return 0

        @pl.when(steps > 0)
        def _():
            fetch(0)

        @pl.when(steps > 1)
        def _():
            fetch(1)

        if first:
            st_ref[:, :, : RANK + 128] = jnp.zeros((REQ, HEADS, RANK + 128), jnp.float32)
            st_ref[:, :, RANK + 128 :] = jnp.full((REQ, HEADS, 128), -1e30, jnp.float32)
        else:
            st_ref[...] = old_ref[...]
        lax.fori_loop(0, steps, step, 0)

        @pl.when(steps > 1)
        def _():
            drain(steps % 2)

        @pl.when(steps > 0)
        def _():
            drain((steps + 1) % 2)

        if last:
            o_ref = outs[3]

            def finish(r, _):
                o_ref[r] = (st_ref[r, :, :RANK] / st_ref[r, :, RANK : RANK + 1]).astype(jnp.bfloat16)
                return 0

            lax.fori_loop(0, REQ, finish, 0)

    smem, vmem, anywhere = (pl.BlockSpec(memory_space=m) for m in (pltpu.SMEM, pltpu.VMEM, pl.ANY))
    state_shape = (REQ, HEADS, RANK + 256)
    in_specs = [smem] * 2 + [anywhere] * total + [vmem] * 2 + [anywhere] * 2
    operands = [counts, codes, *parts, q_lat, q_rope_t]
    aliases = {len(operands): 0, len(operands) + 1: 1}
    operands += list(caches)
    if not first:
        in_specs.append(vmem)
        operands.append(state)
    out_specs = [anywhere, anywhere, vmem]
    out_shape = [jax.ShapeDtypeStruct(c.shape, c.dtype) for c in caches] + [jax.ShapeDtypeStruct(state_shape, jnp.float32)]
    if last:
        out_specs.append(vmem)
        out_shape.append(jax.ShapeDtypeStruct((REQ, HEADS, RANK), jnp.bfloat16))
    return pl.pallas_call(
        kernel,
        in_specs=in_specs,
        out_specs=out_specs,
        out_shape=out_shape,
        scratch_shapes=[
            pltpu.VMEM((3, ROWS, 128), jnp.bfloat16),
            pltpu.VMEM((2, UNIT, RANK), jnp.bfloat16),
            pltpu.VMEM((2, ROPE, UNIT), jnp.bfloat16),
            pltpu.SemaphoreType.DMA((3,)),
            pltpu.SemaphoreType.DMA((2,)),
            pltpu.SemaphoreType.DMA((2,)),
        ],
        input_output_aliases=aliases,
        cost_estimate=pl.CostEstimate(flops=2 * 10**8, bytes_accessed=8 * 589824, transcendentals=0),
        name="attend",
    )(*operands)


def blank_caches(lens):
    def kernel(len_ref, c_ref, k_ref, c_zero, k_zero, c_sem, k_sem):
        c_zero[...] = jnp.zeros_like(c_zero)
        k_zero[...] = jnp.zeros_like(k_zero)

        def each(act):
            def block(n, _):
                r, s = n // N, n % N

                @pl.when(len_ref[r] < (s + 1) * SEQ)
                def _():
                    at = pl.ds(pl.multiple_of(s * SEQ, SEQ), SEQ)
                    act(pltpu.make_async_copy(c_zero, c_ref.at[r, at, :], c_sem.at[n]))
                    act(pltpu.make_async_copy(k_zero, k_ref.at[r, :, at], k_sem.at[n]))

                return 0

            lax.fori_loop(0, REQ * N, block, 0)

        each(lambda copy: copy.start())
        each(lambda copy: copy.wait())

    return pl.pallas_call(
        kernel,
        in_specs=[pl.BlockSpec(memory_space=pltpu.SMEM)],
        out_specs=[pl.BlockSpec(memory_space=pl.ANY)] * 2,
        out_shape=[
            jax.ShapeDtypeStruct((REQ, N * SEQ, RANK), jnp.bfloat16),
            jax.ShapeDtypeStruct((REQ, ROPE, N * SEQ), jnp.bfloat16),
        ],
        scratch_shapes=[
            pltpu.VMEM((SEQ, RANK), jnp.bfloat16),
            pltpu.VMEM((ROPE, SEQ), jnp.bfloat16),
            pltpu.SemaphoreType.DMA((REQ * N,)),
            pltpu.SemaphoreType.DMA((REQ * N,)),
        ],
        cost_estimate=pl.CostEstimate(flops=4 * 10**8, bytes_accessed=85 * 10**6, transcendentals=0),
        name="blank",
    )(lens)


def count_units(seq_lens):
    valid = jnp.clip(seq_lens[None, :] - SEQ * jnp.arange(N, dtype=jnp.int32)[:, None], 0, SEQ)
    left = valid.reshape(N, CHIPS, 2, REQ)[..., None] - UNIT * jnp.arange(PER, dtype=jnp.int32)
    left = left.transpose(0, 1, 3, 4, 2).reshape(N, CHIPS, SLOTS)
    return left


def split_place(place):
    return place // (2 * PER), place // 2 % PER, place % 2


def rank_of(have):
    places = jnp.arange(SLOTS, dtype=jnp.int32)
    return jnp.sum((have[:, None, :] & (places[None, :] <= places[:, None])).astype(jnp.int32), axis=-1)


def place_of(rank, slot):
    return jnp.sum((rank[:, None, :] <= slot[:, :, None]).astype(jnp.int32), axis=-1)


def pack_tables(me, left, slot, spill):
    have = left > 0
    places = jnp.arange(SLOTS, dtype=jnp.int32)
    chips = me // 2 ^ jnp.arange(CHIPS)
    mine = have[me][chips]
    rank = rank_of(mine)
    place = place_of(rank, slot)
    to = jnp.broadcast_to(chips[:, None], place.shape)
    if spill is not None:
        other = np.array([0, 1, 3, 2])
        spilt = spill & (place == SLOTS)
        cap = jnp.asarray(PLAN.cap)[me][:, None]
        place = jnp.where(spilt, place_of(rank[other], 2 * cap - 1 - slot), place)
        to = jnp.where(spilt, chips[other][:, None], to)
    final = jnp.max(jnp.where(mine, places, 0), axis=-1, keepdims=True)
    ok = place < SLOTS
    to = jnp.where(ok, to, chips[:, None])
    req, unit, core = split_place(jnp.where(ok, place, final))
    req = (2 * to + core) * REQ + req
    return [req.reshape(-1), unit.reshape(-1), ok.astype(jnp.int32).reshape(-1)]


def unit_codes(me, source, theirs, slot, valid):
    places = jnp.arange(SLOTS, dtype=jnp.int32)
    place = place_of(rank_of(theirs > 0), slot)
    req, unit, core = split_place(place)
    rows = jnp.sum(jnp.where(place[:, :, None] == places, theirs[:, None, :], 0), axis=-1)
    rows = jnp.where(valid & (core == me % 2), jnp.minimum(rows, UNIT), 0)
    return jnp.where(rows > 0, rows * 2**9 + req * 2**5 + source[:, None] * PER + unit, 0)


def attend_tables(me, left, slot, widths, runs, spill):
    part = jnp.arange(N)
    source = me ^ part
    chip = me // 2
    code = unit_codes(me, source, left[source, chip], slot, True)
    starts = np.cumsum([0] + list(widths))[:-1]
    inside = np.concatenate([np.arange(w) for w in widths])
    depth = np.concatenate([np.full(w, i) for run in runs for i, w in enumerate(widths[c] for c in run)])
    extra = jnp.asarray((inside * 2**18 + depth * N * 2**22).astype(np.int32))
    code = jnp.where(code > 0, code + part[:, None] * 2**22 + extra, 0)
    pieces = [code[:, s : s + w].reshape(-1) for w, s in zip(widths, starts)]
    sizes = [N * sum(widths[c] for c in run) for run in runs]
    if spill:
        source = jnp.where(chip == 3, me ^ 4, me ^ 6) ^ jnp.arange(2)
        cap = jnp.asarray(PLAN.cap[:, 2])[source][:, None]
        unused = jnp.arange(ROOM, dtype=jnp.int32)
        spilt = cap - ROOM + unused
        their_need = jnp.sum((left[source, chip ^ 1] > 0).astype(jnp.int32), axis=-1, keepdims=True)
        valid = (chip >= 2) & (spilt >= their_need)
        more = unit_codes(me, source, left[source, chip], 2 * cap - 1 - spilt, valid)
        more = jnp.where(more > 0, more + (N + jnp.arange(2))[:, None] * 2**22 + unused * 2**18, 0)
        pieces.insert(SPILL + 1, more.reshape(-1))
        sizes[SPILL] += 2 * ROOM
    code = jnp.concatenate(pieces)
    first = np.cumsum([0] + sizes)[:-1]
    run_of = np.repeat(np.arange(len(runs)), sizes).astype(np.int32)
    same = jnp.asarray(run_of)[:, None] == jnp.asarray(run_of)[None, :]
    number = jnp.arange(len(run_of), dtype=jnp.int32)
    before = jnp.sum((same & (number[None, :] < number[:, None]) & (code > 0)[None, :]).astype(jnp.int32), axis=-1)
    goes_to = jnp.where(code > 0, jnp.asarray(first[run_of].astype(np.int32)) + before, -1)
    codes = jnp.sum(jnp.where(goes_to[None, :] == number[:, None], code[None, :], 0), axis=-1)
    in_run = jnp.asarray(run_of)[None, :] == jnp.arange(len(runs), dtype=jnp.int32)[:, None]
    return codes, jnp.sum((in_run & (code > 0)[None, :]).astype(jnp.int32), axis=-1), first


def pairs(sources, hop):
    return [(s, s ^ hop) for s in sources]


def send(x, pairs):
    return lax.ppermute(x, "x", pairs)


def runs_of(count):
    return [(c,) for c in range(count - 2)] + [(count - 2, count - 1)]


def run_plan(me, left, own_lens, weights, q_lat, q_rope_t):
    plan = PLAN
    widths = [chunk[0] for chunk in plan.chunks]
    count = len(widths)
    runs = runs_of(count)
    spill = np.zeros((N, CHIPS, SLOTS), bool)
    spill[np.ix_(SPILLERS, (2, 3), range(plan.starts[SPILL], plan.starts[SPILL] + ROOM))] = True
    pack_tabs = pack_tables(me, left, jnp.asarray(plan.slot)[me], jnp.asarray(spill)[me])
    part = jnp.arange(N)
    codes, counts, first = attend_tables(me, left, jnp.asarray(plan.slot)[me ^ part, part // 2], widths, runs, True)
    caches = blank_caches(own_lens)
    landed, owns, twins = [], [], []
    after = []
    for c, (width, kind, along, across, diagonal) in enumerate(plan.chunks):
        staged = norm_pack(width, int(plan.starts[c]), SLOTS, pack_tabs, *weights, after)
        after = [staged[0]]
        sends = list(staged)
        if c >= DEPTH:
            sends, landed[c - DEPTH] = lax.optimization_barrier((sends, landed[c - DEPTH]))
        owns.append(sends[0])
        twins.append(send(sends[0], pairs(ALL, 1)))
        far = send(sends[3], pairs(ALL, 4) if kind == "relay" else pairs(diagonal, 6))
        near = send(sends[1], pairs(UP, 2) + pairs(LOW, 1) if along == UP else pairs(along, 2))
        over = send(sends[2], pairs(across, 4))
        landed.append([near, over, far])
    state = None
    for number, run in enumerate(runs):
        parts = []
        for c in run:
            near, over, far = landed[c]
            if plan.chunks[c][1] == "relay":
                far = send(far, pairs(LOW, 2) + pairs(UP, 1))
                far, landed[c + 1] = lax.optimization_barrier((far, landed[c + 1]))
            parts += [owns[c], twins[c]]
            for x in (near, over, far):
                parts += [x, send(x, pairs(ALL, 1))]
            if c == SPILL:
                x = send(jnp.where(me // 2 == 3, over, far), pairs(LOW, 2) + pairs(UP, 1))
                x, landed[c + 1] = lax.optimization_barrier((x, landed[c + 1]))
                parts += [x, send(x, pairs(ALL, 1))]
        got = attend(number, int(first[number]), number == 0, number == len(runs) - 1, counts, codes, parts, q_lat, q_rope_t, caches, state)
        caches, state = got[:2], got[2]
    return got


def run_extra(step, cap, me, left, weights, q_lat, q_rope_t, caches, state):
    more = step * EXTRA + jnp.arange(EXTRA, dtype=jnp.int32)
    part = jnp.arange(N)
    slot = cap[me][:, None] + more
    staged = norm_pack(EXTRA, 0, EXTRA, pack_tables(me, left, slot, None), *weights, [])
    slot = cap[me ^ part, part // 2][:, None] + more
    codes, counts, _ = attend_tables(me, left, slot, [EXTRA], [(0,)], False)
    parts = []
    for q, x in enumerate(staged):
        x = lax.ppermute(x, "x", pairs(ALL, 2 * q)) if q else x
        parts += [x, lax.ppermute(x, "x", pairs(ALL, 1))]
    return attend(0, 0, False, True, counts, codes, parts, q_lat, q_rope_t, caches, state)


def local_step(c_raw, k_raw, norm_gain, rope_cos, rope_sin, seq_lens, q_lat, q_rope):
    me = lax.axis_index("x")
    left = count_units(seq_lens)
    own_lens = lax.dynamic_slice_in_dim(seq_lens, me * REQ, REQ)
    weights = (c_raw, jnp.swapaxes(k_raw, 1, 2), norm_gain[None, :], rope_cos.T, rope_sin.T)
    q_rope_t = jnp.swapaxes(q_rope, 1, 2)
    done = run_plan(me, left, own_lens, weights, q_lat, q_rope_t)
    need = jnp.sum((left > 0).astype(jnp.int32), axis=-1)
    to = np.arange(N)[:, None] // 2 ^ np.arange(CHIPS)
    need = jnp.sum(need[:, None, :] * jnp.asarray(to[:, :, None] == np.arange(CHIPS)), axis=-1)
    spills = np.isin(np.arange(N), SPILLERS)[:, None] & np.isin(np.arange(CHIPS), (2, 3))
    room = jnp.clip(jnp.asarray(PLAN.cap) - need[:, np.array([0, 1, 3, 2])], 0, ROOM)
    cap = jnp.asarray(PLAN.cap) + jnp.where(jnp.asarray(spills), room, 0)
    steps = (jnp.maximum(jnp.max(need - cap), 0) + EXTRA - 1) // EXTRA

    def body(carry):
        step, c_cache, k_cache_t, state, _ = carry
        return step + 1, *run_extra(step, cap, me, left, weights, q_lat, q_rope_t, (c_cache, k_cache_t), state)

    _, c_cache, k_cache_t, _, o_lat = lax.while_loop(lambda carry: carry[0] < steps, body, (jnp.int32(0), *done))
    return c_cache, jnp.swapaxes(k_cache_t, 1, 2), o_lat


def solution(mesh):
    seq_spec = P("dp", "x", None)
    req_spec = P(("dp", "x"), None, None)
    return jax.shard_map(
        local_step,
        mesh=mesh,
        in_specs=(seq_spec, seq_spec, P(None), P("x", None), P("x", None), P("dp"), req_spec, req_spec),
        out_specs=(req_spec, req_spec, req_spec),
        check_vma=False,
    )
```

```python
import jax
import jax.numpy as jnp
import numpy as np
from jax import lax
from jax.experimental import pallas as pl
from jax.experimental.pallas import tpu as pltpu
from jax.sharding import PartitionSpec as P

NORM_EPS = 1e-6
N = 8
CHIPS = 4
REQ = 12
SEQ = 768
RANK = 512
ROPE = 64
HEADS = 128
UNIT = 256
PER = SEQ // UNIT
PIECES = RANK // 128
HALVES = UNIT // 128
ROWS = PIECES * UNIT + HALVES * ROPE
SLOTS = 2 * REQ * PER
NONE = 10**6
ATTN_SCALE = (RANK + ROPE) ** -0.5
DEPTH = 2


class Plan:
    def __init__(self, chunks):
        self.chunks = chunks
        self.starts = np.cumsum([0] + [c[0] for c in chunks])[:-1]
        assert sum(c[0] for c in chunks) == SLOTS
        self.slot = np.full((N, CHIPS, SLOTS), NONE, np.int32)
        self.cap = np.zeros((N, CHIPS), np.int32)
        for s in range(N):
            for q in range(CHIPS):
                for chunk, start in zip(chunks, self.starts):
                    width = chunk[0]
                    if q == 0 or s in chunk[q + 1]:
                        self.slot[s, q, start : start + width] = self.cap[s, q] + np.arange(width)
                        self.cap[s, q] += width


ALL = (0, 1, 2, 3, 4, 5, 6, 7)
UP = (0, 1, 2, 3)
LOW = (4, 5, 6, 7)


NO_CHIP1 = (0, 1, 4, 5, 6, 7)
NO_3 = (0, 1, 2, 4, 5, 6, 7)


def direct(width):
    return width, "direct", ALL, ALL, ALL


def relay(width):
    return width, "relay", UP, ALL, UP


def no_chip1(width):
    return width, "direct", ALL, NO_CHIP1, NO_CHIP1


def no_3(width):
    return width, "direct", ALL, NO_3, NO_3


def end(width):
    return width, "direct", UP, ALL, UP


PLAN = Plan(
    [direct(2), direct(4), direct(6), relay(6), no_chip1(6), relay(4), no_3(6)]
    + [direct(8)] * 3
    + [direct(6), end(4), end(2), end(2)]
)
EXTRA = 4


def norm_pack(width, start, stride, tabs, c_raw, k_t, gain, cos_t, sin_t, after):
    steps = CHIPS * width

    def kernel(req_ref, unit_ref, ok_ref, c_ref, k_ref, g_ref, cos_ref, sin_ref, *refs):
        outs, (buf, sem) = refs[len(after) : len(after) + CHIPS], refs[-2:]
        n = pl.program_id(0)
        q, j = n // width, n % width
        ok_at = lambda m: ok_ref[m // width * stride + start + m % width] > 0
        drain = lambda m: pltpu.make_async_copy(buf.at[m % 2], outs[0].at[0], sem.at[m % 2]).wait()
        slot = n % 2

        @pl.when((n >= 2) & ok_at(jnp.maximum(n - 2, 0)))
        def _():
            drain(n)

        @pl.when(ok_at(n))
        def _():
            key = k_ref[0].astype(jnp.float32)
            lo, hi = key[: ROPE // 2], key[ROPE // 2 :]
            cos, sin = cos_ref[...], sin_ref[...]
            rot = jnp.concatenate([lo * cos - hi * sin, hi * cos + lo * sin], axis=0).astype(jnp.bfloat16)
            for p in range(HALVES):
                at = PIECES * UNIT + p * ROPE
                buf[slot, at : at + ROPE, :] = rot[:, p * 128 : (p + 1) * 128]
                x = c_ref[0, p * 128 : (p + 1) * 128, :].astype(jnp.float32)
                inv = lax.rsqrt(jnp.mean(x * x, axis=-1, keepdims=True) + NORM_EPS)
                y = (x * inv * g_ref[...].astype(jnp.float32)).astype(jnp.bfloat16)
                for i in range(PIECES):
                    at = i * UNIT + p * 128
                    buf[slot, at : at + 128, :] = y[:, i * 128 : (i + 1) * 128]
            for mine in range(CHIPS):

                @pl.when(q == mine)
                def _(mine=mine):
                    pltpu.make_async_copy(buf.at[slot], outs[mine].at[j], sem.at[slot]).start()

        @pl.when(n == steps - 1)
        def _():
            @pl.when(ok_at(n - 1))
            def _():
                drain(n - 1)

            @pl.when(ok_at(n))
            def _():
                drain(n)

    def at(n):
        return n // width * stride + start + n % width

    grid_spec = pltpu.PrefetchScalarGridSpec(
        num_scalar_prefetch=3,
        grid=(steps,),
        in_specs=[
            pl.BlockSpec((1, UNIT, RANK), lambda n, req, unit, ok: (req[at(n)], unit[at(n)], 0)),
            pl.BlockSpec((1, ROPE, UNIT), lambda n, req, unit, ok: (req[at(n)], 0, unit[at(n)])),
            pl.BlockSpec((1, RANK), lambda n, *_: (0, 0)),
            pl.BlockSpec((ROPE // 2, UNIT), lambda n, req, unit, ok: (0, unit[at(n)])),
            pl.BlockSpec((ROPE // 2, UNIT), lambda n, req, unit, ok: (0, unit[at(n)])),
        ]
        + [pl.BlockSpec(memory_space=pl.ANY)] * len(after),
        out_specs=[pl.BlockSpec(memory_space=pl.ANY)] * CHIPS,
        scratch_shapes=[pltpu.VMEM((2, ROWS, 128), jnp.bfloat16), pltpu.SemaphoreType.DMA((2,))],
    )
    return pl.pallas_call(
        kernel,
        grid_spec=grid_spec,
        out_shape=[jax.ShapeDtypeStruct((width, ROWS, 128), jnp.bfloat16)] * CHIPS,
        cost_estimate=pl.CostEstimate(flops=width * 10**8, bytes_accessed=width * 4 * 589824, transcendentals=0),
        name="norm_pack",
    )(*tabs, c_raw, k_t, gain, cos_t, sin_t, *after)


def attend(chunk, start, first, last, counts, codes, parts, q_lat, q_rope_t, caches, state):
    total = len(parts)

    def kernel(count_ref, code_ref, *refs):
        part_refs, (qa_ref, qr_ref) = refs[:total], refs[total : total + 2]
        old_ref = None if first else refs[total + 4]
        outs = refs[total + (4 if first else 5) :]
        c_out, k_out, st_ref = outs[:3]
        buf, c_buf, k_buf, in_sem, c_sem, k_sem = outs[-6:]
        steps = count_ref[chunk]

        def fetch(n):
            code = code_ref[start + n]
            part, place = code // 2**22, code // 2**18 % 16
            for k in range(total):

                @pl.when(part == k)
                def _(k=k):
                    pltpu.make_async_copy(part_refs[k].at[place], buf.at[n % 3], in_sem.at[n % 3]).start()

        def drain(slot):
            pltpu.make_async_copy(c_buf.at[slot], c_out.at[0, pl.ds(0, UNIT), :], c_sem.at[slot]).wait()
            pltpu.make_async_copy(k_buf.at[slot], k_out.at[0, :, pl.ds(0, UNIT)], k_sem.at[slot]).wait()

        def step(n, _):
            code = code_ref[start + n]
            left, r = code // 2**9 % 2**9, code // 2**5 % 16
            at = pl.ds(pl.multiple_of(code % 2**5 * UNIT, UNIT), UNIT)
            slot = n % 2

            @pl.when(n + 2 < steps)
            def _():
                fetch(n + 2)

            pltpu.make_async_copy(part_refs[0].at[0], buf.at[n % 3], in_sem.at[n % 3]).wait()

            @pl.when(n >= 2)
            def _():
                drain(slot)

            row_ok = lax.broadcasted_iota(jnp.int32, (UNIT, 1), 0) < left
            lane_ok = lax.broadcasted_iota(jnp.int32, (1, UNIT), 1) < left
            for i in range(PIECES):
                piece = jnp.where(row_ok, buf[n % 3, i * UNIT : (i + 1) * UNIT, :].astype(jnp.float32), 0.0)
                c_buf[slot, :, i * 128 : (i + 1) * 128] = piece.astype(jnp.bfloat16)
            for p in range(HALVES):
                base = PIECES * UNIT + p * ROPE
                key = buf[n % 3, base : base + ROPE, :].astype(jnp.float32)
                key = jnp.where(lane_ok[:, p * 128 : (p + 1) * 128], key, 0.0)
                k_buf[slot, :, p * 128 : (p + 1) * 128] = key.astype(jnp.bfloat16)
            pltpu.make_async_copy(c_buf.at[slot], c_out.at[r, at, :], c_sem.at[slot]).start()
            pltpu.make_async_copy(k_buf.at[slot], k_out.at[r, :, at], k_sem.at[slot]).start()

            c = c_buf[slot]
            scores = lax.dot_general(qa_ref[r], c, (((1,), (1,)), ((), ())), preferred_element_type=jnp.float32)
            scores += lax.dot_general(qr_ref[r], k_buf[slot], (((0,), (0,)), ((), ())), preferred_element_type=jnp.float32)
            scores = jnp.where(lane_ok, scores * ATTN_SCALE, -1e30)
            l_old = st_ref[r, :, RANK : RANK + 1]
            m_old = st_ref[r, :, RANK + 128 : RANK + 129]
            m_new = jnp.maximum(m_old, jnp.max(scores, axis=-1, keepdims=True))
            weights = jnp.exp(scores - m_new)
            decay = jnp.exp(m_old - m_new)
            l_new = l_old * decay + jnp.sum(weights, axis=-1, keepdims=True)
            st_ref[r, :, RANK : RANK + 128] = jnp.broadcast_to(l_new, (HEADS, 128))
            st_ref[r, :, RANK + 128 :] = jnp.broadcast_to(m_new, (HEADS, 128))
            st_ref[r, :, :RANK] = st_ref[r, :, :RANK] * decay + jnp.dot(
                weights.astype(jnp.bfloat16), c, preferred_element_type=jnp.float32
            )
            return 0

        @pl.when(steps > 0)
        def _():
            fetch(0)

        @pl.when(steps > 1)
        def _():
            fetch(1)

        if first:
            st_ref[:, :, : RANK + 128] = jnp.zeros((REQ, HEADS, RANK + 128), jnp.float32)
            st_ref[:, :, RANK + 128 :] = jnp.full((REQ, HEADS, 128), -1e30, jnp.float32)
        else:
            st_ref[...] = old_ref[...]
        lax.fori_loop(0, steps, step, 0)

        @pl.when(steps > 1)
        def _():
            drain(steps % 2)

        @pl.when(steps > 0)
        def _():
            drain((steps + 1) % 2)

        if last:
            o_ref = outs[3]

            def finish(r, _):
                o_ref[r] = (st_ref[r, :, :RANK] / st_ref[r, :, RANK : RANK + 1]).astype(jnp.bfloat16)
                return 0

            lax.fori_loop(0, REQ, finish, 0)

    smem, vmem, anywhere = (pl.BlockSpec(memory_space=m) for m in (pltpu.SMEM, pltpu.VMEM, pl.ANY))
    state_shape = (REQ, HEADS, RANK + 256)
    in_specs = [smem] * 2 + [anywhere] * total + [vmem] * 2 + [anywhere] * 2
    operands = [counts, codes, *parts, q_lat, q_rope_t]
    aliases = {len(operands): 0, len(operands) + 1: 1}
    operands += list(caches)
    if not first:
        in_specs.append(vmem)
        operands.append(state)
    out_specs = [anywhere, anywhere, vmem]
    out_shape = [jax.ShapeDtypeStruct(c.shape, c.dtype) for c in caches] + [jax.ShapeDtypeStruct(state_shape, jnp.float32)]
    if last:
        out_specs.append(vmem)
        out_shape.append(jax.ShapeDtypeStruct((REQ, HEADS, RANK), jnp.bfloat16))
    return pl.pallas_call(
        kernel,
        in_specs=in_specs,
        out_specs=out_specs,
        out_shape=out_shape,
        scratch_shapes=[
            pltpu.VMEM((3, ROWS, 128), jnp.bfloat16),
            pltpu.VMEM((2, UNIT, RANK), jnp.bfloat16),
            pltpu.VMEM((2, ROPE, UNIT), jnp.bfloat16),
            pltpu.SemaphoreType.DMA((3,)),
            pltpu.SemaphoreType.DMA((2,)),
            pltpu.SemaphoreType.DMA((2,)),
        ],
        input_output_aliases=aliases,
        cost_estimate=pl.CostEstimate(flops=2 * 10**8, bytes_accessed=8 * 589824, transcendentals=0),
        name="attend",
    )(*operands)


def blank_caches(lens):
    def kernel(len_ref, c_ref, k_ref, c_zero, k_zero, c_sem, k_sem):
        c_zero[...] = jnp.zeros_like(c_zero)
        k_zero[...] = jnp.zeros_like(k_zero)

        def each(act):
            def block(n, _):
                r, s = n // N, n % N

                @pl.when(len_ref[r] < (s + 1) * SEQ)
                def _():
                    at = pl.ds(pl.multiple_of(s * SEQ, SEQ), SEQ)
                    act(pltpu.make_async_copy(c_zero, c_ref.at[r, at, :], c_sem.at[n]))
                    act(pltpu.make_async_copy(k_zero, k_ref.at[r, :, at], k_sem.at[n]))

                return 0

            lax.fori_loop(0, REQ * N, block, 0)

        each(lambda copy: copy.start())
        each(lambda copy: copy.wait())

    return pl.pallas_call(
        kernel,
        in_specs=[pl.BlockSpec(memory_space=pltpu.SMEM)],
        out_specs=[pl.BlockSpec(memory_space=pl.ANY)] * 2,
        out_shape=[
            jax.ShapeDtypeStruct((REQ, N * SEQ, RANK), jnp.bfloat16),
            jax.ShapeDtypeStruct((REQ, ROPE, N * SEQ), jnp.bfloat16),
        ],
        scratch_shapes=[
            pltpu.VMEM((SEQ, RANK), jnp.bfloat16),
            pltpu.VMEM((ROPE, SEQ), jnp.bfloat16),
            pltpu.SemaphoreType.DMA((REQ * N,)),
            pltpu.SemaphoreType.DMA((REQ * N,)),
        ],
        cost_estimate=pl.CostEstimate(flops=4 * 10**8, bytes_accessed=85 * 10**6, transcendentals=0),
        name="blank",
    )(lens)


def count_units(seq_lens):
    valid = jnp.clip(seq_lens[None, :] - SEQ * jnp.arange(N, dtype=jnp.int32)[:, None], 0, SEQ)
    left = valid.reshape(N, CHIPS, 2, REQ)[..., None] - UNIT * jnp.arange(PER, dtype=jnp.int32)
    left = left.transpose(0, 1, 3, 4, 2).reshape(N, CHIPS, SLOTS)
    return left


def split_place(place):
    return place // (2 * PER), place // 2 % PER, place % 2


def pack_tables(me, left, slot):
    have = left > 0
    places = jnp.arange(SLOTS, dtype=jnp.int32)
    chips = me // 2 ^ jnp.arange(CHIPS)
    mine = have[me][chips]
    rank = jnp.sum((mine[:, None, :] & (places[None, :] <= places[:, None])).astype(jnp.int32), axis=-1)
    place = jnp.sum((rank[:, None, :] <= slot[:, :, None]).astype(jnp.int32), axis=-1)
    final = jnp.max(jnp.where(mine, places, 0), axis=-1, keepdims=True)
    req, unit, core = split_place(jnp.minimum(place, final))
    req = (2 * chips[:, None] + core) * REQ + req
    return [req.reshape(-1), unit.reshape(-1), (place < SLOTS).astype(jnp.int32).reshape(-1)]


def attend_tables(me, left, slot, widths, runs):
    places = jnp.arange(SLOTS, dtype=jnp.int32)
    part = jnp.arange(N)
    source = me ^ part
    theirs = left[source, me // 2]
    rank = jnp.sum(((theirs > 0)[:, None, :] & (places[None, :] <= places[:, None])).astype(jnp.int32), axis=-1)
    place = jnp.sum((rank[:, None, :] <= slot[:, :, None]).astype(jnp.int32), axis=-1)
    req, unit, core = split_place(place)
    rows = jnp.sum(jnp.where(place[:, :, None] == places, theirs[:, None, :], 0), axis=-1)
    rows = jnp.where(core == me % 2, jnp.minimum(rows, UNIT), 0)
    starts = np.cumsum([0] + list(widths))[:-1]
    inside = np.concatenate([np.arange(w) for w in widths])
    depth = np.concatenate([np.full(w, i) for run in runs for i, w in enumerate(widths[c] for c in run)])
    code = part[:, None] * 2**22 + rows * 2**9 + req * 2**5 + source[:, None] * PER + unit
    code = jnp.where(rows > 0, code + jnp.asarray((inside * 2**18 + depth * N * 2**22).astype(np.int32)), 0)
    code = jnp.concatenate([code[:, s : s + w].reshape(-1) for w, s in zip(widths, starts)])
    sizes = [N * sum(widths[c] for c in run) for run in runs]
    first = np.cumsum([0] + sizes)[:-1]
    run_of = np.repeat(np.arange(len(runs)), sizes).astype(np.int32)
    same = jnp.asarray(run_of)[:, None] == jnp.asarray(run_of)[None, :]
    number = jnp.arange(len(run_of), dtype=jnp.int32)
    before = jnp.sum((same & (number[None, :] < number[:, None]) & (code > 0)[None, :]).astype(jnp.int32), axis=-1)
    goes_to = jnp.where(code > 0, jnp.asarray(first[run_of].astype(np.int32)) + before, -1)
    codes = jnp.sum(jnp.where(goes_to[None, :] == number[:, None], code[None, :], 0), axis=-1)
    in_run = jnp.asarray(run_of)[None, :] == jnp.arange(len(runs), dtype=jnp.int32)[:, None]
    return codes, jnp.sum((in_run & (code > 0)[None, :]).astype(jnp.int32), axis=-1), first


def pairs(sources, hop):
    return [(s, s ^ hop) for s in sources]


def send(x, pairs):
    return lax.ppermute(x, "x", pairs)


def runs_of(count):
    return [(c,) for c in range(count - 2)] + [(count - 2, count - 1)]


def run_plan(me, left, own_lens, weights, q_lat, q_rope_t):
    plan = PLAN
    widths = [chunk[0] for chunk in plan.chunks]
    count = len(widths)
    runs = runs_of(count)
    pack_tabs = pack_tables(me, left, jnp.asarray(plan.slot)[me])
    part = jnp.arange(N)
    codes, counts, first = attend_tables(me, left, jnp.asarray(plan.slot)[me ^ part, part // 2], widths, runs)
    caches = blank_caches(own_lens)
    landed, owns, twins = [], [], []
    after = []
    for c, (width, kind, along, across, diagonal) in enumerate(plan.chunks):
        staged = norm_pack(width, int(plan.starts[c]), SLOTS, pack_tabs, *weights, after)
        after = [staged[0]]
        sends = list(staged)
        if c >= DEPTH:
            sends, landed[c - DEPTH] = lax.optimization_barrier((sends, landed[c - DEPTH]))
        owns.append(sends[0])
        twins.append(send(sends[0], pairs(ALL, 1)))
        far = send(sends[3], pairs(ALL, 4) if kind == "relay" else pairs(diagonal, 6))
        near = send(sends[1], pairs(UP, 2) + pairs(LOW, 1) if along == UP else pairs(ALL, 2))
        over = send(sends[2], pairs(across, 4))
        landed.append([near, over, far])
    state = None
    for number, run in enumerate(runs):
        parts = []
        for c in run:
            near, over, far = landed[c]
            if plan.chunks[c][1] == "relay":
                far = send(far, pairs(LOW, 2) + pairs(UP, 1))
                far, landed[c + 1] = lax.optimization_barrier((far, landed[c + 1]))
            parts += [owns[c], twins[c]]
            for x in (near, over, far):
                parts += [x, send(x, pairs(ALL, 1))]
        got = attend(number, int(first[number]), number == 0, number == len(runs) - 1, counts, codes, parts, q_lat, q_rope_t, caches, state)
        caches, state = got[:2], got[2]
    return got


def run_extra(step, me, left, weights, q_lat, q_rope_t, caches, state):
    cap = jnp.asarray(PLAN.cap)
    more = step * EXTRA + jnp.arange(EXTRA, dtype=jnp.int32)
    part = jnp.arange(N)
    slot = cap[me][:, None] + more
    staged = norm_pack(EXTRA, 0, EXTRA, pack_tables(me, left, slot), *weights, [])
    slot = cap[me ^ part, part // 2][:, None] + more
    codes, counts, _ = attend_tables(me, left, slot, [EXTRA], [(0,)])
    parts = []
    for q, x in enumerate(staged):
        x = lax.ppermute(x, "x", pairs(ALL, 2 * q)) if q else x
        parts += [x, lax.ppermute(x, "x", pairs(ALL, 1))]
    return attend(0, 0, False, True, counts, codes, parts, q_lat, q_rope_t, caches, state)


def local_step(c_raw, k_raw, norm_gain, rope_cos, rope_sin, seq_lens, q_lat, q_rope):
    me = lax.axis_index("x")
    left = count_units(seq_lens)
    own_lens = lax.dynamic_slice_in_dim(seq_lens, me * REQ, REQ)
    weights = (c_raw, jnp.swapaxes(k_raw, 1, 2), norm_gain[None, :], rope_cos.T, rope_sin.T)
    q_rope_t = jnp.swapaxes(q_rope, 1, 2)
    done = run_plan(me, left, own_lens, weights, q_lat, q_rope_t)
    need = jnp.sum((left > 0).astype(jnp.int32), axis=-1)
    cap = np.stack([[PLAN.cap[s, (s // 2) ^ chip] for chip in range(CHIPS)] for s in range(N)])
    steps = (jnp.maximum(jnp.max(need - jnp.asarray(cap)), 0) + EXTRA - 1) // EXTRA

    def body(carry):
        step, c_cache, k_cache_t, state, _ = carry
        return step + 1, *run_extra(step, me, left, weights, q_lat, q_rope_t, (c_cache, k_cache_t), state)

    _, c_cache, k_cache_t, _, o_lat = lax.while_loop(lambda carry: carry[0] < steps, body, (jnp.int32(0), *done))
    return c_cache, jnp.swapaxes(k_cache_t, 1, 2), o_lat


def solution(mesh):
    seq_spec = P("dp", "x", None)
    req_spec = P(("dp", "x"), None, None)
    return jax.shard_map(
        local_step,
        mesh=mesh,
        in_specs=(seq_spec, seq_spec, P(None), P("x", None), P("x", None), P("dp"), req_spec, req_spec),
        out_specs=(req_spec, req_spec, req_spec),
        check_vma=False,
    )
```
